256 devices in a mesh: row: 8 (over x, core), col: 8 (over z), depth: 4 (over y).
Axes of the slice: x: 4, y: 4, z: 8, core: 2. Of those that a mesh axis runs over, the one named last changes fastest.
Arguments:
- x_blocks: bfloat16 [256, 4, 256, 256], P(('row', 'col'), 'depth'), may hold values from -0.25 to 0.25
- x_columns: int32 [256, 4], P(('row', 'col'), 'depth'), may hold values from 0 to 255, as said below
- h_blocks: bfloat16 [256, 4, 256, 256], P(('row', 'col')), may hold values from -6 to 6
- h_columns: int32 [256, 4], P(('row', 'col')), may hold values from 0 to 255, as said below
- p_columns: int32 [256, 4], P(('row', 'col')), may hold values from 0 to 255, as said below
- q_columns: int32 [256, 4], P(('row', 'col')), may hold values from 0 to 255, as said below
Outputs:
- product_p: bfloat16 [256, 4, 256, 256], P(('row', 'col'), 'depth')
- product_q: bfloat16 [256, 4, 256, 256], P(('row', 'col'), 'depth')
The draws below stay inside these ranges and needn't reach their ends.
Inputs may be any that keep to these rules, and one draw needn't show every extreme that they name: `x_columns`: row i holds 4 distinct block columns (i + o) mod 256 with -2 <= o <= 2. `h_columns`: row i holds 4 distinct block columns (i + o) mod 256 with -2 <= o <= 2. `p_columns`: row i holds 4 distinct block columns (i + o) mod 256 with -4 <= o <= 4. `q_columns`: row i holds 4 distinct block columns (i + o) mod 256 with -6 <= o <= 6.
All inputs are finite; a program needn't handle non-finite values.
Results may differ from the reference program's by a relative error of at most 0.0049.
Values may be sent and summed in bfloat16 or wider, within the bound.
No kernel may reach another device: no remote copies, remote signals or barrier semaphores. Data moves between devices by JAX's collectives and lax.ppermute only.
A program may use at most 64 MiB of HBM per device.

```python
import jax
import jax.numpy as jnp
from jax import lax

BLOCK = 256
SLOTS = 4
REACH = 2
PSLOTS = 4
QSLOTS = 4
NBLOCKS = 256


def banded_columns(key, count, spread):
    offsets = jax.vmap(lambda sub_key: jax.random.permutation(sub_key, 2 * spread + 1)[:count])(jax.random.split(key, NBLOCKS))
    rows_index = jnp.arange(NBLOCKS, dtype=jnp.int32)[:, None]
    return jnp.mod(rows_index + offsets.astype(jnp.int32) - spread, NBLOCKS).astype(jnp.int32)


def draw_x_columns(key, part):
    return banded_columns(jax.random.fold_in(key, 11), SLOTS, REACH)


def draw_h_columns(key, part):
    return banded_columns(jax.random.fold_in(key, 22), SLOTS, REACH)


def draw_p_columns(key, part):
    return banded_columns(jax.random.fold_in(key, 33), PSLOTS, 2 * REACH)


def draw_q_columns(key, part):
    return banded_columns(jax.random.fold_in(key, 44), QSLOTS, 3 * REACH)


def block_levels(key, shape, pieces, smallest, largest):
    gain = 1.0
    for axis_at, parts in pieces:
        draws = jax.random.uniform(jax.random.fold_in(jax.random.fold_in(key, 6), axis_at), (parts,), jnp.float32, smallest / len(pieces), largest / len(pieces))
        gain = gain * jnp.repeat(jnp.exp(draws), shape[axis_at] // parts).reshape((-1,) + (1,) * (len(shape) - 1 - axis_at))
    return gain


def centred(own_key, extent, scale, bound, cuts=(), held_as=jnp.bfloat16):
    values = scale * jax.random.normal(own_key, extent, jnp.float32)
    if cuts:
        values = values * block_levels(own_key, extent, cuts, -0.22, 0.18)
    return jnp.clip(values, -bound, bound).astype(held_as)


def setup_inputs(seed: int = 0) -> dict:
    splits = jax.random.split(jax.random.key(seed), 7)
    return {
        "x_blocks": centred(splits[0], (NBLOCKS, SLOTS, BLOCK, BLOCK), (2 * BLOCK) ** -0.5, 0.25, ((0, 64), (1, 4))),
        "x_columns": draw_x_columns(jax.random.fold_in(splits[6], 71), 0),
        "h_blocks": centred(splits[2], (NBLOCKS, SLOTS, BLOCK, BLOCK), 1.0, 6.0, ((0, 64),)),
        "h_columns": draw_h_columns(jax.random.fold_in(splits[6], 71), 0),
        "p_columns": draw_p_columns(jax.random.fold_in(splits[6], 71), 0),
        "q_columns": draw_q_columns(jax.random.fold_in(splits[6], 71), 0),
    }


def sparse_rows(left_blocks, left_columns, wanted, right_blocks, right_columns):
    fetched = right_blocks[left_columns].astype(jnp.float32)
    fetched_columns = right_columns[left_columns]
    chosen_mask = (fetched_columns[:, :, None] == wanted[None, None, :]).astype(jnp.float32)
    chosen = jnp.einsum('kmp,kmbc->kpbc', chosen_mask, fetched, precision=lax.Precision.HIGHEST)
    return jnp.einsum('kab,kpbc->pac', left_blocks.astype(jnp.float32), chosen, precision=lax.Precision.HIGHEST)


def reference(x_blocks, x_columns, h_blocks, h_columns, p_columns, q_columns):
    def first_row(items):
        left_blocks, left_columns, wanted = items
        return sparse_rows(left_blocks, left_columns, wanted, h_blocks, h_columns).astype(jnp.bfloat16)

    product_p = lax.map(first_row, (x_blocks, x_columns, p_columns))

    def second_row(items):
        left_blocks, left_columns, wanted = items
        return sparse_rows(left_blocks, left_columns, wanted, x_blocks, x_columns).astype(jnp.bfloat16)

    product_q = lax.map(second_row, (product_p, p_columns, q_columns))
    return product_p, product_q
```

```python
import functools

import jax
import jax.numpy as jnp
from jax import lax
from jax.experimental import pallas as pl
from jax.experimental.pallas import tpu as pltpu
from jax.sharding import PartitionSpec as P

REACH = 2
PAD = 16
BF16, F32, I32 = jnp.bfloat16, jnp.float32, jnp.int32


ANY = pl.BlockSpec(memory_space=pl.ANY)
SMEM = pl.BlockSpec(memory_space=pltpu.SMEM)
VMEM = pl.BlockSpec(memory_space=pltpu.VMEM)


def low_half(shape):
    return lax.broadcasted_iota(I32, shape, 1) < 64


def swapped(tile):
    return pltpu.roll(tile.astype(F32), 64, 1).astype(tile.dtype)


def copies(pairs, sems):
    made = [pltpu.make_async_copy(a, b, sems.at[n]) for n, (a, b) in enumerate(pairs)]
    for copy in made:
        copy.start()
    return made


def slice_kernel(meta, *refs):
    *tiles, out = refs
    upper = meta[0] % 2
    for pair in range(len(tiles) // 2):
        a, b = tiles[2 * pair], tiles[2 * pair + 1]

        @pl.when(upper == 0)
        def _():
            left, right = a[...], swapped(b[...])
            out[:, 128 * pair : 128 * pair + 128] = jnp.where(low_half(left.shape), left, right)

        @pl.when(upper == 1)
        def _():
            left, right = swapped(a[...]), b[...]
            out[:, 128 * pair : 128 * pair + 128] = jnp.where(low_half(left.shape), left, right)


def column_slices(payloads, d):
    rows, width = payloads[0].shape
    spec = pl.BlockSpec((rows, 128), lambda n, meta: (0, meta[0] // 2))
    return pl.pallas_call(
        slice_kernel,
        grid_spec=pltpu.PrefetchScalarGridSpec(
            num_scalar_prefetch=1,
            grid=(1,),
            in_specs=[spec] * len(payloads),
            out_specs=pl.BlockSpec((rows, width), lambda n, meta: (0, 0)),
        ),
        out_shape=jax.ShapeDtypeStruct((rows, width), BF16),
        name="column_slices",
    )(d[None], *payloads)


def p_kernel(rows, all_rows, meta, pc, hc, x0, x1, x2, x3, h, lo, hi, full, mine, xbuf, hbuf, cols, tabv, tab, sems):
    size = x0.shape[1]
    body = rows * size
    edge = lo.shape[0] - PAD
    slots = h.shape[0] // size // rows
    near = edge // size // slots
    total = 2 * edge + h.shape[0]
    d, first = meta[0], meta[1]
    xs = (x0, x1, x2, x3)
    small = copies(
        [(x.at[pl.ds(body, PAD)], cols.at[n]) for n, x in enumerate(xs)]
        + [(e.at[pl.ds(edge, PAD)], cols.at[4 + n]) for n, e in enumerate((lo, hi))],
        sems,
    )
    large = copies(
        [(x.at[pl.ds(0, body)], xbuf.at[n]) for n, x in enumerate(xs)]
        + [
            (lo.at[pl.ds(0, edge)], hbuf.at[pl.ds(0, edge)]),
            (h, hbuf.at[pl.ds(edge, h.shape[0])]),
            (hi.at[pl.ds(0, edge)], hbuf.at[pl.ds(edge + h.shape[0], edge)]),
        ],
        sems.at[pl.ds(8, 8)],
    )
    hbuf[pl.ds(total, size), :] = jnp.zeros((size, size), BF16)
    for copy in small:
        copy.wait()
    for n in range(6):
        tabv[8 * n : 8 * n + 8, :] = cols[n, 0:8, 0:128].astype(F32).astype(I32)
    move = pltpu.make_async_copy(tabv, tab, sems.at[7])
    move.start()
    move.wait()
    for copy in large:
        copy.wait()

    @pl.loop(0, rows * slots)
    def _(at):
        i, p = at // slots, at % slots
        want = pc[i, p]
        acc = jnp.zeros((size, size), F32)
        for k in range(4):
            j = lax.rem(tab[8 * k + i, 0] - first + near + all_rows, all_rows)
            low, high = j < near, j >= near + rows
            pick = jnp.int32(total)
            for m in range(slots):
                column = jnp.where(
                    low,
                    tab[32 + jnp.clip(j, 0, near - 1), m],
                    jnp.where(
                        high,
                        tab[40 + jnp.clip(j - near - rows, 0, near - 1), m],
                        hc[jnp.clip(j - near, 0, rows - 1), m],
                    ),
                )
                pick = jnp.where(column == want, (j * slots + m) * size, pick)
            block = hbuf[pl.ds(pl.multiple_of(pick, size), size), :]
            left = xbuf[k, pl.ds(pl.multiple_of(i * size, size), size), :]
            acc += jnp.dot(left, block, preferred_element_type=F32)
        value = acc.astype(BF16)
        full[at] = value

        @pl.when(p == d)
        def _():
            mine[i] = value


def p_product(meta, pc, hc, xs, h, lo, hi, all_rows):
    rows, slots = pc.shape
    size = h.shape[-1]
    flat = h.reshape(-1, size)
    return pl.pallas_call(
        functools.partial(p_kernel, rows, all_rows),
        in_specs=[SMEM] * 3 + [ANY] * 7,
        out_specs=[VMEM, VMEM],
        out_shape=[
            jax.ShapeDtypeStruct((rows * slots, size, size), BF16),
            jax.ShapeDtypeStruct((rows, size, size), BF16),
        ],
        scratch_shapes=[
            pltpu.VMEM((4, rows * size, size), BF16),
            pltpu.VMEM((flat.shape[0] + 2 * (lo.shape[0] - PAD) + size, size), BF16),
            pltpu.VMEM((6, PAD, size), BF16),
            pltpu.VMEM((48, 128), I32),
            pltpu.SMEM((48, 128), I32),
            pltpu.SemaphoreType.DMA((16,)),
        ],
        cost_estimate=pl.CostEstimate(
            flops=2 * rows * slots * 4 * size**3, bytes_accessed=9 << 20, transcendentals=0
        ),
        name="p_product",
    )(meta, pc, hc, *xs, flat, lo, hi)


def q_kernel(rows, all_rows, meta, pc, qc, lo, own, hi, full, s0, s1, s2, s3, raw, tiles, pbuf, tabv, tab, res, sems):
    size = lo.shape[1]
    body = rows * size
    d, first = meta[0], meta[1]
    slots = pc.shape[1]
    moves = copies([(lo, raw.at[0]), (own, raw.at[1]), (hi, raw.at[2]), (full, pbuf)], sems)
    empty = 12 * slots * size
    tiles[pl.ds(empty, size), :] = jnp.zeros((size, 128), BF16)
    for copy in moves[:3]:
        copy.wait()
    for n in range(3):
        tabv[8 * n : 8 * n + 8, :] = raw[n, body : body + 8, :].astype(F32).astype(I32)
    move = pltpu.make_async_copy(tabv, tab, sems.at[4])
    move.start()
    for n in range(3):
        for r in range(rows):
            for t in range(2):
                tile = raw[n, r * size : r * size + size, 128 * t : 128 * t + 128]
                base = (((n * rows + r) * 2 + t) * 2) * size
                tiles[base : base + size, :] = tile
                tiles[base + size : base + 2 * size, :] = swapped(tile)
    move.wait()
    moves[3].wait()
    mask = low_half((size, 128))

    for i in range(rows):
        acc = jnp.zeros((size, size), F32)
        for p in range(slots):
            j = lax.rem(pc[i, p] - first + rows + all_rows, all_rows)
            tab_row = 8 * (j // rows) + j % rows
            picks = []
            for q in range(slots):
                half = (q + i) % 2
                pick = jnp.int32(empty)
                for m in range(slots):
                    spot = (j * 4 + (m // 2) * 2 + (m % 2 != half)) * size
                    pick = jnp.where(tab[tab_row, 64 * m] == qc[i, q], spot, pick)
                picks.append(tiles[pl.ds(pl.multiple_of(pick, size), size), :])
            pairs = [(picks[0], picks[1]), (picks[2], picks[3])]
            if i % 2:
                pairs = [(b, a) for a, b in pairs]
            right = jnp.concatenate([jnp.where(mask, a, b) for a, b in pairs], axis=1)
            acc += jnp.dot(pbuf[i * slots + p], right, preferred_element_type=F32)
        value = acc.astype(BF16)
        res[2 * i] = value[:, :128]
        res[2 * i + 1] = value[:, 128:]
    for o, out in enumerate((s0, s1, s2, s3)):
        q = lax.rem(d + o, 4)
        even = mask == (q % 2 == 0)
        for e in range(rows // 2):
            out[e * size : e * size + size, :] = jnp.where(
                even, res[4 * e + q // 2], res[4 * e + 2 + q // 2]
            )


def q_product(meta, pc, qc, lo, own, hi, full, all_rows):
    rows, slots = pc.shape
    size = own.shape[1]
    return pl.pallas_call(
        functools.partial(q_kernel, rows, all_rows),
        in_specs=[SMEM] * 3 + [ANY] * 4,
        out_specs=[VMEM] * 4,
        out_shape=[jax.ShapeDtypeStruct((rows // 2 * size, 128), BF16)] * 4,
        scratch_shapes=[
            pltpu.VMEM((3, own.shape[0], size), BF16),
            pltpu.VMEM(((12 * slots + 1) * size, 128), BF16),
            pltpu.VMEM(full.shape, BF16),
            pltpu.VMEM((24, size), I32),
            pltpu.SMEM((24, size), I32),
            pltpu.VMEM((2 * rows, size, 128), BF16),
            pltpu.SemaphoreType.DMA((5,)),
        ],
        cost_estimate=pl.CostEstimate(
            flops=2 * rows * slots * size**3, bytes_accessed=5 << 20, transcendentals=0
        ),
        name="q_product",
    )(meta, pc, qc, lo, own, hi, full)


def join_kernel(meta, t0, t1, t2, t3, out, held):
    d = meta[0]
    size = out.shape[1]
    for o, t in enumerate((t0, t1, t2, t3)):
        held[lax.rem(d - o + 4, 4)] = t[...]
    mask = low_half((size, 128))
    for side in range(2):

        @pl.when(d % 2 == side)
        def _():
            for i in range(out.shape[0]):
                rows = slice(i // 2 * size, i // 2 * size + size)
                for t in range(2):
                    a, b = held[2 * t, rows], held[2 * t + 1, rows]
                    if (side + i) % 2 == 0:
                        b = swapped(b)
                    else:
                        a = swapped(a)
                    out[i, :, 128 * t : 128 * t + 128] = jnp.where(mask, a, b)


def join(meta, parts, rows, size):
    return pl.pallas_call(
        join_kernel,
        in_specs=[SMEM] + [VMEM] * 4,
        out_specs=VMEM,
        out_shape=jax.ShapeDtypeStruct((rows, size, size), BF16),
        scratch_shapes=[pltpu.VMEM((4, *parts[0].shape), BF16)],
        name="join",
    )(meta, *parts)


def local(x_blocks, x_columns, h_blocks, h_columns, p_columns, q_columns):
    rows, _, size, _ = x_blocks.shape
    groups = lax.axis_size(("row", "col"))
    depth = lax.axis_size("depth")
    all_rows = rows * groups
    d = lax.axis_index("depth").astype(I32)
    first = lax.axis_index(("row", "col")).astype(I32) * rows
    meta = jnp.stack([d, first])

    up = [(g, (g + 1) % groups) for g in range(groups)]
    down = [(b, a) for a, b in up]

    def payload(blocks, table):
        pad = jnp.zeros((PAD - table.shape[0], size), BF16)
        return jnp.concatenate([blocks.reshape(-1, size), table.astype(BF16), pad])

    def h_payload(part, table):
        wide = jnp.pad(table, ((0, 0), (0, size - table.shape[1])))
        return payload(part, wide)

    x_own = payload(x_blocks, jnp.broadcast_to(x_columns, (rows, size)))
    xs = [x_own] + [
        lax.ppermute(x_own, "depth", [(s, (s + o) % depth) for s in range(depth)])
        for o in range(1, depth)
    ]
    h_lo = lax.ppermute(
        h_payload(h_blocks[rows - REACH :], h_columns[rows - REACH :]), ("row", "col"), up
    )
    h_hi = lax.ppermute(h_payload(h_blocks[:REACH], h_columns[:REACH]), ("row", "col"), down)

    slices = column_slices(xs, d)
    s_lo = lax.ppermute(slices, ("row", "col"), up)
    s_hi = lax.ppermute(slices, ("row", "col"), down)
    full, mine = p_product(meta, p_columns, h_columns, xs, h_blocks, h_lo, h_hi, all_rows)
    parts = q_product(meta, p_columns, q_columns, s_lo, slices, s_hi, full, all_rows)
    parts = [parts[0]] + [
        lax.ppermute(parts[o], "depth", [(s, (s + o) % depth) for s in range(depth)])
        for o in range(1, depth)
    ]
    product_q = join(meta, parts, rows, size)
    return mine[:, None], product_q[:, None]


def solution(mesh):
    in_specs = (
        P(("row", "col"), "depth", None, None),
        P(("row", "col"), "depth"),
        P(("row", "col"), None, None, None),
        P(("row", "col"), None),
        P(("row", "col"), None),
        P(("row", "col"), None),
    )
    out_specs = (P(("row", "col"), "depth", None, None), P(("row", "col"), "depth", None, None))
    return jax.shard_map(local, mesh=mesh, in_specs=in_specs, out_specs=out_specs, check_vma=False)
```

```python
import functools

import jax
import jax.numpy as jnp
from jax import lax
from jax.experimental import pallas as pl
from jax.experimental.pallas import tpu as pltpu
from jax.sharding import PartitionSpec as P

REACH = 2
PAD = 16
BF16, F32, I32 = jnp.bfloat16, jnp.float32, jnp.int32


ANY = pl.BlockSpec(memory_space=pl.ANY)
SMEM = pl.BlockSpec(memory_space=pltpu.SMEM)
VMEM = pl.BlockSpec(memory_space=pltpu.VMEM)
HBM = pl.BlockSpec(memory_space=pltpu.HBM)


def low_half(shape):
    return lax.broadcasted_iota(I32, shape, 1) < 64


def swapped(tile):
    return pltpu.roll(tile.astype(F32), 64, 1).astype(tile.dtype)


def vmem(x):
    return pltpu.with_memory_space_constraint(x, pltpu.VMEM)


def hbm(x):
    return pltpu.with_memory_space_constraint(x, pltpu.HBM)


def copies(pairs, sems):
    made = [pltpu.make_async_copy(a, b, sems.at[n]) for n, (a, b) in enumerate(pairs)]
    for copy in made:
        copy.start()
    return made


def pack_kernel(x_columns, h_columns, x, h, x_low, x_high, h_up, h_down, xc, hc, sems):
    cut, size = x_low.shape
    tail = x_high.shape[0] - PAD
    edge = h_up.shape[0] - PAD
    small = copies([(x_columns, xc), (h_columns, hc)], sems.at[pl.ds(4, 2)])
    moves = copies(
        [
            (x.at[pl.ds(0, cut)], x_low),
            (x.at[pl.ds(cut, tail)], x_high.at[pl.ds(0, tail)]),
            (h.at[pl.ds(h.shape[0] - edge, edge)], h_up.at[pl.ds(0, edge)]),
            (h.at[pl.ds(0, edge)], h_down.at[pl.ds(0, edge)]),
        ],
        sems,
    )
    shape = (PAD, size)
    row, lane = lax.broadcasted_iota(I32, shape, 0), lax.broadcasted_iota(I32, shape, 1)
    rows, slots = hc.shape
    for move in small:
        move.wait()
    table = jnp.zeros(shape, I32)
    for r in range(rows):
        table = jnp.where(row == r, xc[0, r], table)
    x_high[tail:, :] = table.astype(F32).astype(BF16)
    for out, start in ((h_up, rows - REACH), (h_down, 0)):
        table = jnp.zeros(shape, I32)
        for r in range(REACH):
            for m in range(slots):
                table = jnp.where((row == r) & (lane == m), hc[start + r, m], table)
        out[edge:, :] = table.astype(F32).astype(BF16)
    for move in moves:
        move.wait()


def pack(x_blocks, x_columns, h_blocks, h_columns):
    rows, slots, size, _ = h_blocks.shape
    x, h = x_blocks.reshape(-1, size), h_blocks.reshape(-1, size)
    half = rows // 2 * size
    edge = pltpu.VMEM((REACH * slots * size + PAD, size), BF16)
    return pl.pallas_call(
        pack_kernel,
        in_specs=[HBM] * 4,
        out_specs=[VMEM] * 4,
        out_shape=[
            pltpu.VMEM((half, size), BF16),
            pltpu.VMEM((x.shape[0] - half + PAD, size), BF16),
            edge,
            edge,
        ],
        scratch_shapes=[
            pltpu.SMEM((1, rows), I32),
            pltpu.SMEM((rows, slots), I32),
            pltpu.SemaphoreType.DMA((6,)),
        ],
        compiler_params=pltpu.CompilerParams(vmem_limit_bytes=8 << 20),
        name="pack",
    )(*[hbm(a) for a in (x_columns.T, h_columns, x, h)])


def slice_kernel(*refs):
    *parts, out = refs
    d = lax.axis_index("depth")
    tile = pl.ds(pl.multiple_of(d // 2 * 128, 128), 128)
    cut = parts[0].shape[0]
    for upper in range(2):

        @pl.when(d % 2 == upper)
        def _():
            for n, rows in enumerate((slice(0, cut), slice(cut, out.shape[0]))):
                for pair in range(2):
                    a, b = parts[4 * pair + n][:, tile], parts[4 * pair + 2 + n][:, tile]
                    a, b = (swapped(a), b) if upper else (a, swapped(b))
                    out[rows, 128 * pair : 128 * pair + 128] = jnp.where(low_half(a.shape), a, b)


def column_slices(payloads):
    low, high = payloads[:2]
    return pl.pallas_call(
        slice_kernel,
        in_specs=[VMEM] * 8,
        out_specs=VMEM,
        out_shape=pltpu.VMEM((low.shape[0] + high.shape[0], low.shape[1]), BF16),
        compiler_params=pltpu.CompilerParams(vmem_limit_bytes=8 << 20),
        name="column_slices",
    )(*[vmem(x) for x in payloads])


def p_kernel(rows, all_rows, pc, hc, *refs):
    *xs, h, lo, hi, full, mine, hbuf, tabv, tab, sems = refs
    d, first = lax.axis_index("depth"), lax.axis_index(("row", "col")) * rows
    cut, size = xs[0].shape
    body = rows * size
    edge = lo.shape[0] - PAD
    slots = h.shape[0] // size // rows
    near = edge // size // slots
    total = 2 * edge + h.shape[0]
    large = copies(
        [
            (lo.at[pl.ds(0, edge)], hbuf.at[pl.ds(0, edge)]),
            (h, hbuf.at[pl.ds(edge, h.shape[0])]),
            (hi.at[pl.ds(0, edge)], hbuf.at[pl.ds(edge + h.shape[0], edge)]),
        ],
        sems,
    )
    tables = [x[body - cut :, :128] for x in xs[1::2]] + [lo[edge:, :128], hi[edge:, :128]]
    for n, table in enumerate(tables):
        tabv[8 * n : 8 * n + 8, :] = table[:8].astype(F32).astype(I32)
    move = pltpu.make_async_copy(tabv, tab, sems.at[3])
    move.start()
    hbuf[pl.ds(total, size), :] = jnp.zeros((size, size), BF16)
    move.wait()
    for copy in large:
        copy.wait()

    for i in range(rows):
        part, at = i * size // cut, i * size % cut
        lefts = [xs[2 * k + part][at : at + size, :] for k in range(4)]

        @pl.loop(0, slots)
        def _(p):
            want = pc[i, p]
            acc = jnp.zeros((size, size), F32)
            for k in range(4):
                j = lax.rem(tab[8 * k + i, 0] - first + near + all_rows, all_rows)
                low, high = j < near, j >= near + rows
                pick = jnp.int32(total)
                for m in range(slots):
                    column = jnp.where(
                        low,
                        tab[32 + jnp.clip(j, 0, near - 1), m],
                        jnp.where(
                            high,
                            tab[40 + jnp.clip(j - near - rows, 0, near - 1), m],
                            hc[jnp.clip(j - near, 0, rows - 1), m],
                        ),
                    )
                    pick = jnp.where(column == want, (j * slots + m) * size, pick)
                block = hbuf[pl.ds(pl.multiple_of(pick, size), size), :]
                acc += jnp.dot(lefts[k], block, preferred_element_type=F32)
            value = acc.astype(BF16)
            full[i * slots + p] = value

            @pl.when(p == d)
            def _():
                mine[i] = value


def p_product(pc, hc, xs, h, lo, hi, all_rows):
    rows, slots = pc.shape
    size = h.shape[-1]
    flat = h.reshape(-1, size)
    return pl.pallas_call(
        functools.partial(p_kernel, rows, all_rows),
        in_specs=[SMEM] * 2 + [VMEM] * 11,
        out_specs=[VMEM, VMEM],
        out_shape=[
            pltpu.VMEM((rows * slots, size, size), BF16),
            jax.ShapeDtypeStruct((rows, size, size), BF16),
        ],
        scratch_shapes=[
            pltpu.VMEM((flat.shape[0] + 2 * (lo.shape[0] - PAD) + size, size), BF16),
            pltpu.VMEM((48, 128), I32),
            pltpu.SMEM((48, 128), I32),
            pltpu.SemaphoreType.DMA((4,)),
        ],
        cost_estimate=pl.CostEstimate(
            flops=2 * rows * slots * 4 * size**3, bytes_accessed=9 << 20, transcendentals=0
        ),
        compiler_params=pltpu.CompilerParams(vmem_limit_bytes=24 << 20),
        name="p_product",
    )(pc, hc, *[vmem(x) for x in xs], vmem(flat), vmem(lo), vmem(hi))


def q_kernel(rows, all_rows, pc, qc, lo, own, hi, full, s0, s1, s2, s3, tiles, tabv, tab, res, sem):
    size = lo.shape[1]
    body = rows * size
    slots = pc.shape[1]
    raw = (lo, own, hi)
    d, first = lax.axis_index("depth"), lax.axis_index(("row", "col")) * rows
    for n in range(3):
        tabv[8 * n : 8 * n + 8, :] = raw[n][body : body + 8, :].astype(F32).astype(I32)
    move = pltpu.make_async_copy(tabv, tab, sem)
    move.start()
    empty = 12 * slots * size
    tiles[pl.ds(empty, size), :] = jnp.zeros((size, 128), BF16)
    for n in range(3):
        for r in range(rows):
            for t in range(2):
                tile = raw[n][r * size : r * size + size, 128 * t : 128 * t + 128]
                base = (((n * rows + r) * 2 + t) * 2) * size
                tiles[base : base + size, :] = tile
                tiles[base + size : base + 2 * size, :] = swapped(tile)
    move.wait()
    mask = low_half((size, 128))

    for i in range(rows):
        acc = jnp.zeros((size, size), F32)
        for p in range(slots):
            j = lax.rem(pc[i, p] - first + rows + all_rows, all_rows)
            tab_row = 8 * (j // rows) + j % rows
            picks = []
            for q in range(slots):
                half = (q + i) % 2
                pick = jnp.int32(empty)
                for m in range(slots):
                    spot = (j * 4 + (m // 2) * 2 + (m % 2 != half)) * size
                    pick = jnp.where(tab[tab_row, 64 * m] == qc[i, q], spot, pick)
                picks.append(tiles[pl.ds(pl.multiple_of(pick, size), size), :])
            pairs = [(picks[0], picks[1]), (picks[2], picks[3])]
            if i % 2:
                pairs = [(b, a) for a, b in pairs]
            right = jnp.concatenate([jnp.where(mask, a, b) for a, b in pairs], axis=1)
            acc += jnp.dot(full[i * slots + p], right, preferred_element_type=F32)
        value = acc.astype(BF16)
        res[2 * i] = value[:, :128]
        res[2 * i + 1] = value[:, 128:]
    for o, out in enumerate((s0, s1, s2, s3)):
        q = lax.rem(d + o, 4)
        even = mask == (q % 2 == 0)
        for e in range(rows // 2):
            out[e * size : e * size + size, :] = jnp.where(
                even, res[4 * e + q // 2], res[4 * e + 2 + q // 2]
            )


def q_product(pc, qc, lo, own, hi, full, all_rows):
    rows, slots = pc.shape
    size = own.shape[1]
    return pl.pallas_call(
        functools.partial(q_kernel, rows, all_rows),
        in_specs=[SMEM] * 2 + [VMEM] * 4,
        out_specs=[VMEM] * 4,
        out_shape=[pltpu.VMEM((rows // 2 * size, 128), BF16)] * 4,
        scratch_shapes=[
            pltpu.VMEM(((12 * slots + 1) * size, 128), BF16),
            pltpu.VMEM((24, size), I32),
            pltpu.SMEM((24, size), I32),
            pltpu.VMEM((2 * rows, size, 128), BF16),
            pltpu.SemaphoreType.DMA,
        ],
        cost_estimate=pl.CostEstimate(
            flops=2 * rows * slots * size**3, bytes_accessed=5 << 20, transcendentals=0
        ),
        compiler_params=pltpu.CompilerParams(vmem_limit_bytes=24 << 20),
        name="q_product",
    )(pc, qc, vmem(lo), vmem(own), vmem(hi), vmem(full))


def join_kernel(t0, t1, t2, t3, out, held):
    size, d = out.shape[1], lax.axis_index("depth")
    for o, t in enumerate((t0, t1, t2, t3)):
        held[lax.rem(d - o + 4, 4)] = t[...]
    mask = low_half((size, 128))
    for side in range(2):

        @pl.when(d % 2 == side)
        def _():
            for i in range(out.shape[0]):
                rows = slice(i // 2 * size, i // 2 * size + size)
                for t in range(2):
                    a, b = held[2 * t, rows], held[2 * t + 1, rows]
                    if (side + i) % 2 == 0:
                        b = swapped(b)
                    else:
                        a = swapped(a)
                    out[i, :, 128 * t : 128 * t + 128] = jnp.where(mask, a, b)


def join(parts, rows, size):
    return pl.pallas_call(
        join_kernel,
        in_specs=[VMEM] * 4,
        out_specs=VMEM,
        out_shape=jax.ShapeDtypeStruct((rows, size, size), BF16),
        scratch_shapes=[pltpu.VMEM((4, *parts[0].shape), BF16)],
        compiler_params=pltpu.CompilerParams(vmem_limit_bytes=8 << 20),
        name="join",
    )(*[vmem(x) for x in parts])


def local(x_blocks, x_columns, h_blocks, h_columns, p_columns, q_columns):
    rows, _, size, _ = x_blocks.shape
    groups = lax.axis_size(("row", "col"))
    depth = lax.axis_size("depth")
    all_rows = rows * groups
    up = [(g, (g + 1) % groups) for g in range(groups)]
    down = [(b, a) for a, b in up]

    def turn(x, o):
        return lax.ppermute(x, "depth", [(s, (s + o) % depth) for s in range(depth)])

    x_low, x_high, h_up, h_down = pack(x_blocks, x_columns, h_blocks, h_columns)
    low_one, high_three = turn(x_low, 1), turn(x_high, 3)
    h_lo = lax.ppermute(h_up, ("row", "col"), up)
    h_hi = lax.ppermute(h_down, ("row", "col"), down)
    high_one, low_three = turn(x_high, 1), turn(x_low, 3)
    low_two, high_two = turn(low_one, 1), turn(high_three, 3)
    xs = [x_low, x_high, low_one, high_one, low_two, high_two, low_three, high_three]

    slices = column_slices(xs)
    s_lo = lax.ppermute(slices, ("row", "col"), up)
    s_hi = lax.ppermute(slices, ("row", "col"), down)
    full, mine = p_product(p_columns, h_columns, xs, h_blocks, h_lo, h_hi, all_rows)
    parts = q_product(p_columns, q_columns, s_lo, slices, s_hi, full, all_rows)
    parts = [parts[0]] + [turn(parts[o], o) for o in range(1, depth)]
    product_q = join(parts, rows, size)
    return mine[:, None], product_q[:, None]


def solution(mesh):
    in_specs = (
        P(("row", "col"), "depth", None, None),
        P(("row", "col"), "depth"),
        P(("row", "col"), None, None, None),
        P(("row", "col"), None),
        P(("row", "col"), None),
        P(("row", "col"), None),
    )
    out_specs = (P(("row", "col"), "depth", None, None), P(("row", "col"), "depth", None, None))
    return jax.shard_map(local, mesh=mesh, in_specs=in_specs, out_specs=out_specs, check_vma=False)
```

```python
import functools

import jax
import jax.numpy as jnp
from jax import lax
from jax.experimental import pallas as pl
from jax.experimental.pallas import tpu as pltpu
from jax.sharding import PartitionSpec as P


REACH = 2
PAD = 16
BF16, F32, I32 = jnp.bfloat16, jnp.float32, jnp.int32


ANY = pl.BlockSpec(memory_space=pl.ANY)
SMEM = pl.BlockSpec(memory_space=pltpu.SMEM)
VMEM = pl.BlockSpec(memory_space=pltpu.VMEM)
HBM = pl.BlockSpec(memory_space=pltpu.HBM)


def low_half(shape):
    return lax.broadcasted_iota(I32, shape, 1) < 64


def swapped(tile):
    return pltpu.roll(tile.astype(F32), 64, 1).astype(tile.dtype)


def vmem(x):
    return pltpu.with_memory_space_constraint(x, pltpu.VMEM)


def hbm(x):
    return pltpu.with_memory_space_constraint(x, pltpu.HBM)


def copies(pairs, sems):
    made = [pltpu.make_async_copy(a, b, sems.at[n]) for n, (a, b) in enumerate(pairs)]
    for copy in made:
        copy.start()
    return made


def pack_kernel(x_columns, h_columns, x, h, x_low, x_high, h_up, h_down, xc, hc, sems):
    cut, size = x_low.shape
    tail = x_high.shape[0] - PAD
    edge = h_up.shape[0] - PAD
    rows, slots = hc.shape
    d, straight = lax.axis_index("depth"), slots - 1
    small = copies([(x_columns, xc), (h_columns, hc)], sems.at[pl.ds(14, 2)])
    moves = copies(
        [
            (x.at[pl.ds(0, cut)], x_low),
            (x.at[pl.ds(cut, tail)], x_high.at[pl.ds(0, tail)]),
        ]
        + [
            (
                h.at[pl.ds(pl.multiple_of(((start + r) * slots + lax.rem(d + way * n + slots, slots)) * size, size), size)],
                out.at[pl.ds((r * straight + n) * size, size)],
            )
            for out, start, way in ((h_up, rows - REACH, 1), (h_down, 0, -1))
            for r in range(REACH)
            for n in range(straight)
        ],
        sems,
    )
    shape = (PAD, size)
    row, lane = lax.broadcasted_iota(I32, shape, 0), lax.broadcasted_iota(I32, shape, 1)
    for move in small:
        move.wait()
    table = jnp.zeros(shape, I32)
    for r in range(rows):
        table = jnp.where(row == r, xc[0, r], table)
    x_high[tail:, :] = table.astype(F32).astype(BF16)
    for out, start in ((h_up, rows - REACH), (h_down, 0)):
        table = jnp.zeros(shape, I32)
        for r in range(REACH):
            for m in range(slots):
                table = jnp.where((row == r) & (lane == m), hc[start + r, m], table)
        out[edge:, :] = table.astype(F32).astype(BF16)
    for move in moves:
        move.wait()


def pack(x_blocks, x_columns, h_blocks, h_columns):
    rows, slots, size, _ = h_blocks.shape
    x, h = x_blocks.reshape(-1, size), h_blocks.reshape(-1, size)
    half = rows // 2 * size
    edge = pltpu.VMEM((REACH * (slots - 1) * size + PAD, size), BF16)
    return pl.pallas_call(
        pack_kernel,
        in_specs=[HBM] * 4,
        out_specs=[VMEM] * 4,
        out_shape=[
            pltpu.VMEM((half, size), BF16),
            pltpu.VMEM((x.shape[0] - half + PAD, size), BF16),
            edge,
            edge,
        ],
        scratch_shapes=[
            pltpu.SMEM((1, rows), I32),
            pltpu.SMEM((rows, slots), I32),
            pltpu.SemaphoreType.DMA((16,)),
        ],
        compiler_params=pltpu.CompilerParams(vmem_limit_bytes=8 << 20),
        name="pack",
    )(*[hbm(a) for a in (x_columns.T, h_columns, x, h)])


def slice_kernel(a_low, a_high, b_low, b_high, out):
    d = lax.axis_index("depth")
    tile = pl.ds(pl.multiple_of(d // 2 * 128, 128), 128)
    cut = a_low.shape[0]
    for upper in range(2):

        @pl.when(d % 2 == upper)
        def _():
            for left, right, rows in ((a_low, b_low, slice(0, cut)), (a_high, b_high, slice(cut, None))):
                a, b = left[:, tile], right[:, tile]
                a, b = (swapped(a), b) if upper else (a, swapped(b))
                out[rows, :] = jnp.where(low_half(a.shape), a, b)


def column_slices(payloads):
    low, high = payloads[:2]
    return pl.pallas_call(
        slice_kernel,
        in_specs=[VMEM] * 4,
        out_specs=VMEM,
        out_shape=pltpu.VMEM((low.shape[0] + high.shape[0], 128), BF16),
        compiler_params=pltpu.CompilerParams(vmem_limit_bytes=8 << 20),
        name="column_slices",
    )(*[vmem(x) for x in payloads])


def first_slot_kernel(lo, hi, out_lo, out_hi):
    size = lo.shape[1]
    step = (lo.shape[0] - PAD) // REACH
    for source, out in ((lo, out_lo), (hi, out_hi)):
        for r in range(REACH):
            out[r * size : r * size + size, :] = source[r * step : r * step + size, :]


def first_slots(lo, hi):
    size = lo.shape[1]
    return pl.pallas_call(
        first_slot_kernel,
        in_specs=[VMEM] * 2,
        out_specs=[VMEM] * 2,
        out_shape=[pltpu.VMEM((REACH * size, size), BF16)] * 2,
        compiler_params=pltpu.CompilerParams(vmem_limit_bytes=4 << 20),
        name="first_slots",
    )(vmem(lo), vmem(hi))


def table_to_scalars(tables, tabv, tab, sem):
    for n, table in enumerate(tables):
        tabv[8 * n : 8 * n + 8, :] = table.astype(F32).astype(I32)
    move = pltpu.make_async_copy(tabv, tab, sem)
    move.start()
    move.wait()


def x_tables(xs):
    return [x[x.shape[0] - PAD : x.shape[0] - PAD + 8, :128] for x in xs[1::2]]


def x_row(xs, k, i):
    cut, size = xs[0].shape
    at = i * size % cut
    return xs[2 * k + i * size // cut][at : at + size, :]


def own_block(column, first, all_rows, want, hc, h, zero):
    rows, slots = hc.shape
    size = h.shape[1]
    j = lax.rem(column - first + all_rows, all_rows)
    row = jnp.minimum(j, rows - 1)
    pick, found = jnp.int32(0), jnp.bool_(False)
    for m in range(slots):
        match = (hc[row, m] == want) & (j < rows)
        pick = jnp.where(match, m, pick)
        found = found | match
    spot = pl.multiple_of((row * slots + pick) * size, size)
    return jnp.where(found, h[pl.ds(spot, size), :], zero)


def near_kernel(rows, all_rows, pc, hc, *refs):
    *xs, h, total, tabv, tab, sem = refs
    size = h.shape[1]
    slots = pc.shape[1]
    first = lax.axis_index(("row", "col")) * rows
    table_to_scalars(x_tables(xs), tabv, tab, sem)
    zero = jnp.zeros((size, size), BF16)
    for i in range(rows):
        for p in range(slots):
            acc = jnp.zeros((size, size), F32)
            for k in range(len(xs) // 2):
                block = own_block(tab[8 * k + i, 0], first, all_rows, pc[i, p], hc, h, zero)
                acc += jnp.dot(x_row(xs, k, i), block, preferred_element_type=F32)
            total[i * slots + p] = acc


def near_terms(pc, hc, xs, h, all_rows):
    rows, slots = pc.shape
    size = h.shape[-1]
    return pl.pallas_call(
        functools.partial(near_kernel, rows, all_rows),
        in_specs=[SMEM] * 2 + [VMEM] * (len(xs) + 1),
        out_specs=VMEM,
        out_shape=pltpu.VMEM((rows * slots, size, size), F32),
        scratch_shapes=[
            pltpu.VMEM((4 * len(xs), 128), I32),
            pltpu.SMEM((4 * len(xs), 128), I32),
            pltpu.SemaphoreType.DMA,
        ],
        cost_estimate=pl.CostEstimate(
            flops=rows * slots * len(xs) * size**3, bytes_accessed=9 << 20, transcendentals=0
        ),
        compiler_params=pltpu.CompilerParams(vmem_limit_bytes=8 << 20),
        name="near_terms",
    )(pc, hc, *[vmem(x) for x in xs], vmem(h.reshape(-1, size)))


def far_kernel(rows, all_rows, pc, *refs):
    *xs, lo, hi, lo_side, hi_side, total, full, mine, tabv, tab, sem = refs
    size = lo.shape[1]
    slots = pc.shape[1]
    edge = lo.shape[0] - PAD
    d, first = lax.axis_index("depth"), lax.axis_index(("row", "col")) * rows
    table_to_scalars(
        x_tables(xs) + [e[edge : edge + 8, :128] for e in (lo, hi)], tabv, tab, sem
    )
    zero = jnp.zeros((size, size), BF16)
    for i in range(rows):
        far = [(32 + r, lo, lo_side, r, 1, r - REACH) for r in range(REACH) if r - REACH >= i - REACH]
        far += [(40 + r, hi, hi_side, r, -1, rows + r) for r in range(REACH) if rows + r <= i + REACH]
        lefts = []
        for *_, j in far:
            column = lax.rem(first + j + all_rows, all_rows)
            left = zero
            for k in range(4):
                left = jnp.where(tab[8 * k + i, 0] == column, x_row(xs, k, i), left)
            lefts.append(left)
        for p in range(slots):
            want = pc[i, p]
            acc = total[i * slots + p]
            for left, (at, straight, side, r, way, _) in zip(lefts, far):
                pick, found = jnp.int32(0), jnp.bool_(False)
                for m in range(slots):
                    match = tab[at, m] == want
                    pick = jnp.where(match, m, pick)
                    found = found | match
                n = lax.rem(way * (pick - d) + slots, slots)
                spot = (r * (slots - 1) + jnp.minimum(n, slots - 2)) * size
                block = jnp.where(
                    n < slots - 1,
                    straight[pl.ds(pl.multiple_of(spot, size), size), :],
                    side[r * size : r * size + size, :],
                )
                acc += jnp.dot(left, jnp.where(found, block, zero), preferred_element_type=F32)
            full[i * slots + p] = acc.astype(BF16)
        mine[i] = full[i * slots + d]


def far_terms(pc, xs, edges, total, all_rows):
    rows, slots = pc.shape
    size = total.shape[-1]
    return pl.pallas_call(
        functools.partial(far_kernel, rows, all_rows),
        in_specs=[SMEM] + [VMEM] * 13,
        out_specs=[VMEM, VMEM],
        out_shape=[
            pltpu.VMEM((rows * slots, size, size), BF16),
            jax.ShapeDtypeStruct((rows, size, size), BF16),
        ],
        scratch_shapes=[
            pltpu.VMEM((48, 128), I32),
            pltpu.SMEM((48, 128), I32),
            pltpu.SemaphoreType.DMA,
        ],
        cost_estimate=pl.CostEstimate(
            flops=2 * 24 * size**3, bytes_accessed=9 << 20, transcendentals=0
        ),
        compiler_params=pltpu.CompilerParams(vmem_limit_bytes=8 << 20),
        name="far_terms",
    )(pc, *[vmem(x) for x in (*xs, *edges, total)])


def q_kernel(rows, all_rows, pc, qc, lo_a, own_a, hi_a, lo_b, own_b, hi_b, full, s0, s1, s2, s3, tiles, tabv, tab, res, sem):
    size = full.shape[1]
    body = rows * size
    slots = pc.shape[1]
    raw = ((lo_a, lo_b), (own_a, own_b), (hi_a, hi_b))
    d, first = lax.axis_index("depth"), lax.axis_index(("row", "col")) * rows
    for n in range(3):
        for t in range(2):
            part = raw[n][t][body : body + 8, :]
            tabv[8 * n : 8 * n + 8, 128 * t : 128 * t + 128] = part.astype(F32).astype(I32)
    move = pltpu.make_async_copy(tabv, tab, sem)
    move.start()
    empty = 12 * slots * size
    tiles[pl.ds(empty, size), :] = jnp.zeros((size, 128), BF16)
    for n in range(3):
        for r in range(rows):
            for t in range(2):
                tile = raw[n][t][r * size : r * size + size, :]
                base = (((n * rows + r) * 2 + t) * 2) * size
                tiles[base : base + size, :] = tile
                tiles[base + size : base + 2 * size, :] = swapped(tile)
    move.wait()
    mask = low_half((size, 128))

    for i in range(rows):
        acc = jnp.zeros((size, size), F32)
        for p in range(slots):
            j = lax.rem(pc[i, p] - first + rows + all_rows, all_rows)
            tab_row = 8 * (j // rows) + j % rows
            picks = []
            for q in range(slots):
                half = (q + i) % 2
                pick = jnp.int32(empty)
                for m in range(slots):
                    spot = (j * 4 + (m // 2) * 2 + (m % 2 != half)) * size
                    pick = jnp.where(tab[tab_row, 64 * m] == qc[i, q], spot, pick)
                picks.append(tiles[pl.ds(pl.multiple_of(pick, size), size), :])
            pairs = [(picks[0], picks[1]), (picks[2], picks[3])]
            if i % 2:
                pairs = [(b, a) for a, b in pairs]
            right = jnp.concatenate([jnp.where(mask, a, b) for a, b in pairs], axis=1)
            acc += jnp.dot(full[i * slots + p], right, preferred_element_type=F32)
        value = acc.astype(BF16)
        res[2 * i] = value[:, :128]
        res[2 * i + 1] = value[:, 128:]
    for o, out in enumerate((s0, s1, s2, s3)):
        q = lax.rem(d + o, 4)
        even = mask == (q % 2 == 0)
        for e in range(rows // 2):
            out[e * size : e * size + size, :] = jnp.where(
                even, res[4 * e + q // 2], res[4 * e + 2 + q // 2]
            )


def q_product(pc, qc, pieces, full, all_rows):
    rows, slots = pc.shape
    size = full.shape[1]
    return pl.pallas_call(
        functools.partial(q_kernel, rows, all_rows),
        in_specs=[SMEM] * 2 + [VMEM] * 7,
        out_specs=[VMEM] * 4,
        out_shape=[pltpu.VMEM((rows // 2 * size, 128), BF16)] * 4,
        scratch_shapes=[
            pltpu.VMEM(((12 * slots + 1) * size, 128), BF16),
            pltpu.VMEM((24, size), I32),
            pltpu.SMEM((24, size), I32),
            pltpu.VMEM((2 * rows, size, 128), BF16),
            pltpu.SemaphoreType.DMA,
        ],
        cost_estimate=pl.CostEstimate(
            flops=2 * rows * slots * size**3, bytes_accessed=5 << 20, transcendentals=0
        ),
        compiler_params=pltpu.CompilerParams(vmem_limit_bytes=24 << 20),
        name="q_product",
    )(pc, qc, *[vmem(x) for x in (*pieces, full)])


def join_kernel(t0, t1, t2, t3, out, held):
    size, d = out.shape[1], lax.axis_index("depth")
    for o, t in enumerate((t0, t1, t2, t3)):
        held[lax.rem(d - o + 4, 4)] = t[...]
    mask = low_half((size, 128))
    for side in range(2):

        @pl.when(d % 2 == side)
        def _():
            for i in range(out.shape[0]):
                rows = slice(i // 2 * size, i // 2 * size + size)
                for t in range(2):
                    a, b = held[2 * t, rows], held[2 * t + 1, rows]
                    if (side + i) % 2 == 0:
                        b = swapped(b)
                    else:
                        a = swapped(a)
                    out[i, :, 128 * t : 128 * t + 128] = jnp.where(mask, a, b)


def join(parts, rows, size):
    return pl.pallas_call(
        join_kernel,
        in_specs=[VMEM] * 4,
        out_specs=VMEM,
        out_shape=jax.ShapeDtypeStruct((rows, size, size), BF16),
        scratch_shapes=[pltpu.VMEM((4, *parts[0].shape), BF16)],
        compiler_params=pltpu.CompilerParams(vmem_limit_bytes=8 << 20),
        name="join",
    )(*[vmem(x) for x in parts])


def local(x_blocks, x_columns, h_blocks, h_columns, p_columns, q_columns):
    rows, _, size, _ = x_blocks.shape
    groups = lax.axis_size(("row", "col"))
    depth = lax.axis_size("depth")
    all_rows = rows * groups
    up = [(g, (g + 1) % groups) for g in range(groups)]
    down = [(b, a) for a, b in up]

    def turn(x, o):
        return lax.ppermute(x, "depth", [(s, (s + o) % depth) for s in range(depth)])

    def shift(x, pairs):
        return lax.ppermute(x, ("row", "col"), pairs)

    x_low, x_high, h_up, h_down = pack(x_blocks, x_columns, h_blocks, h_columns)
    h_lo, h_hi = shift(h_up, up), shift(h_down, down)
    low_one, high_three = turn(x_low, 1), turn(x_high, 3)
    high_one, low_three = turn(x_high, 1), turn(x_low, 3)
    low_two, high_two = turn(low_one, 1), turn(high_three, 3)
    xs = [x_low, x_high, low_one, high_one, low_three, high_three, low_two, high_two]

    a = column_slices(xs[:4])
    a_lo, a_hi = shift(a, up), shift(a, down)
    send_lo, send_hi = first_slots(h_lo, h_hi)
    edges = [h_lo, h_hi, turn(send_lo, 1), turn(send_hi, 3)]
    b = column_slices(xs[4:])
    b_lo, b_hi = shift(b, up), shift(b, down)
    total = near_terms(p_columns, h_columns, xs, h_blocks, all_rows)
    full, mine = far_terms(p_columns, xs, edges, total, all_rows)
    pieces = (a_lo, a, a_hi, b_lo, b, b_hi)
    parts = q_product(p_columns, q_columns, pieces, full, all_rows)
    parts = [parts[0]] + [turn(parts[o], o) for o in range(1, depth)]
    product_q = join(parts, rows, size)
    return mine[:, None], product_q[:, None]


def solution(mesh):
    in_specs = (
        P(("row", "col"), "depth", None, None),
        P(("row", "col"), "depth"),
        P(("row", "col"), None, None, None),
        P(("row", "col"), None),
        P(("row", "col"), None),
        P(("row", "col"), None),
    )
    out_specs = (P(("row", "col"), "depth", None, None), P(("row", "col"), "depth", None, None))
    return jax.shard_map(local, mesh=mesh, in_specs=in_specs, out_specs=out_specs, check_vma=False)
```

```python
import functools

import jax
import jax.numpy as jnp
from jax import lax
from jax.experimental import pallas as pl
from jax.experimental.pallas import tpu as pltpu
from jax.sharding import PartitionSpec as P


REACH = 2
PAD = 16
BF16, F32, I32 = jnp.bfloat16, jnp.float32, jnp.int32


ANY = pl.BlockSpec(memory_space=pl.ANY)
SMEM = pl.BlockSpec(memory_space=pltpu.SMEM)
VMEM = pl.BlockSpec(memory_space=pltpu.VMEM)
HBM = pl.BlockSpec(memory_space=pltpu.HBM)


def low_half(shape):
    return lax.broadcasted_iota(I32, shape, 1) < 64


def swapped(tile):
    return pltpu.roll(tile.astype(F32), 64, 1).astype(tile.dtype)


def vmem(x):
    return pltpu.with_memory_space_constraint(x, pltpu.VMEM)


def hbm(x):
    return pltpu.with_memory_space_constraint(x, pltpu.HBM)


def copies(pairs, sems):
    made = [pltpu.make_async_copy(a, b, sems.at[n]) for n, (a, b) in enumerate(pairs)]
    for copy in made:
        copy.start()
    return made


def pack_kernel(x_columns, h_columns, x, h, x_low, x_high, h_up, h_down, xc, hc, sems):
    cut, size = x_low.shape
    tail = x_high.shape[0] - PAD
    edge = h_up.shape[0] - PAD
    rows, slots = hc.shape
    d, straight = lax.axis_index("depth"), slots - 1
    small = copies([(x_columns, xc), (h_columns, hc)], sems.at[pl.ds(14, 2)])
    moves = copies(
        [
            (x.at[pl.ds(0, cut)], x_low),
            (x.at[pl.ds(cut, tail)], x_high.at[pl.ds(0, tail)]),
        ]
        + [
            (
                h.at[pl.ds(pl.multiple_of(((start + r) * slots + lax.rem(d + way * n + slots, slots)) * size, size), size)],
                out.at[pl.ds((r * straight + n) * size, size)],
            )
            for out, start, way in ((h_up, rows - REACH, 1), (h_down, 0, -1))
            for r in range(REACH)
            for n in range(straight)
        ],
        sems,
    )
    shape = (PAD, size)
    row, lane = lax.broadcasted_iota(I32, shape, 0), lax.broadcasted_iota(I32, shape, 1)
    for move in small:
        move.wait()
    table = jnp.zeros(shape, I32)
    for r in range(rows):
        table = jnp.where(row == r, xc[0, r], table)
    x_high[tail:, :] = table.astype(F32).astype(BF16)
    for out, start in ((h_up, rows - REACH), (h_down, 0)):
        table = jnp.zeros(shape, I32)
        for r in range(REACH):
            for m in range(slots):
                table = jnp.where((row == r) & (lane == m), hc[start + r, m], table)
        out[edge:, :] = table.astype(F32).astype(BF16)
    for move in moves:
        move.wait()


def pack(x_blocks, x_columns, h_blocks, h_columns):
    rows, slots, size, _ = h_blocks.shape
    x, h = x_blocks.reshape(-1, size), h_blocks.reshape(-1, size)
    half = rows // 2 * size
    edge = pltpu.VMEM((REACH * (slots - 1) * size + PAD, size), BF16)
    return pl.pallas_call(
        pack_kernel,
        in_specs=[HBM] * 4,
        out_specs=[VMEM] * 4,
        out_shape=[
            pltpu.VMEM((half, size), BF16),
            pltpu.VMEM((x.shape[0] - half + PAD, size), BF16),
            edge,
            edge,
        ],
        scratch_shapes=[
            pltpu.SMEM((1, rows), I32),
            pltpu.SMEM((rows, slots), I32),
            pltpu.SemaphoreType.DMA((16,)),
        ],
        compiler_params=pltpu.CompilerParams(vmem_limit_bytes=8 << 20),
        name="pack",
    )(*[hbm(a) for a in (x_columns.T, h_columns, x, h)])


TABLE = pltpu.VMEM((16, 128), I32)


def whole(table, parts):
    for n, part in enumerate(parts):
        table[8 * n : 8 * n + 8, :] = part.astype(F32).astype(I32)


def slice_kernel(a_low, a_high, b_low, b_high, out, table):
    d = lax.axis_index("depth")
    tile = pl.ds(pl.multiple_of(d // 2 * 128, 128), 128)
    cut = a_low.shape[0]
    whole(table, [x[x.shape[0] - PAD : x.shape[0] - PAD + 8, :128] for x in (a_high, b_high)])
    for upper in range(2):

        @pl.when(d % 2 == upper)
        def _():
            for left, right, rows in ((a_low, b_low, slice(0, cut)), (a_high, b_high, slice(cut, None))):
                a, b = left[:, tile], right[:, tile]
                a, b = (swapped(a), b) if upper else (a, swapped(b))
                out[rows, :] = jnp.where(low_half(a.shape), a, b)


def column_slices(payloads):
    low, high = payloads[:2]
    return pl.pallas_call(
        slice_kernel,
        in_specs=[VMEM] * 4,
        out_specs=[VMEM, VMEM],
        out_shape=[pltpu.VMEM((low.shape[0] + high.shape[0], 128), BF16), TABLE],
        compiler_params=pltpu.CompilerParams(vmem_limit_bytes=8 << 20),
        name="column_slices",
    )(*[vmem(x) for x in payloads])


def first_slot_kernel(lo, hi, out_lo, out_hi, table):
    size = lo.shape[1]
    whole(table, [x[x.shape[0] - PAD : x.shape[0] - PAD + 8, :128] for x in (lo, hi)])
    step = (lo.shape[0] - PAD) // REACH
    for source, out in ((lo, out_lo), (hi, out_hi)):
        for r in range(REACH):
            out[r * size : r * size + size, :] = source[r * step : r * step + size, :]


def first_slots(lo, hi):
    size = lo.shape[1]
    return pl.pallas_call(
        first_slot_kernel,
        in_specs=[VMEM] * 2,
        out_specs=[VMEM] * 3,
        out_shape=[pltpu.VMEM((REACH * size, size), BF16)] * 2 + [TABLE],
        compiler_params=pltpu.CompilerParams(vmem_limit_bytes=4 << 20),
        name="first_slots",
    )(vmem(lo), vmem(hi))


def x_row(xs, k, i):
    cut, size = xs[0].shape
    at = i * size % cut
    return xs[2 * k + i * size // cut][at : at + size, :]


def own_block(column, first, all_rows, want, hc, h, zero):
    rows, slots = hc.shape
    size = h.shape[1]
    j = lax.rem(column - first + all_rows, all_rows)
    row = jnp.minimum(j, rows - 1)
    pick, found = jnp.int32(0), jnp.bool_(False)
    for m in range(slots):
        match = (hc[row, m] == want) & (j < rows)
        pick = jnp.where(match, m, pick)
        found = found | match
    spot = pl.multiple_of((row * slots + pick) * size, size)
    return jnp.where(found, h[pl.ds(spot, size), :], zero)


def own_kernel(rows, all_rows, pc, hc, xc, low, high, h, total):
    size = h.shape[1]
    slots = pc.shape[1]
    first = lax.axis_index(("row", "col")) * rows
    zero = jnp.zeros((size, size), BF16)
    for i in range(rows):
        for p in range(slots):
            block = own_block(xc[0, i], first, all_rows, pc[i, p], hc, h, zero)
            total[i * slots + p] = jnp.dot(x_row((low, high), 0, i), block, preferred_element_type=F32)


def near_kernel(rows, all_rows, pc, hc, tab_a, tab_b, *refs):
    *xs, h, before, total = refs
    size = h.shape[1]
    slots = pc.shape[1]
    first = lax.axis_index(("row", "col")) * rows
    zero = jnp.zeros((size, size), BF16)
    for i in range(rows):
        for p in range(slots):
            acc = before[i * slots + p]
            for k in range(1, 4):
                column = (tab_a, tab_b)[k // 2][8 * (k % 2) + i, 0]
                block = own_block(column, first, all_rows, pc[i, p], hc, h, zero)
                acc += jnp.dot(x_row(xs, k - 1, i), block, preferred_element_type=F32)
            total[i * slots + p] = acc


def near_terms(kernel, scalars, arrays, all_rows):
    rows, slots = scalars[0].shape
    size = arrays[0].shape[1]
    terms = 3 if len(arrays) > 3 else 1
    return pl.pallas_call(
        functools.partial(kernel, rows, all_rows),
        in_specs=[SMEM] * len(scalars) + [VMEM] * len(arrays),
        out_specs=VMEM,
        out_shape=pltpu.VMEM((rows * slots, size, size), F32),
        cost_estimate=pl.CostEstimate(
            flops=2 * rows * slots * terms * size**3, bytes_accessed=9 << 20, transcendentals=0
        ),
        compiler_params=pltpu.CompilerParams(vmem_limit_bytes=8 << 20),
    )(*scalars, *[vmem(x) for x in arrays])


def far_kernel(rows, all_rows, pc, tab_a, tab_b, tab_h, *refs):
    *xs, lo, hi, lo_side, hi_side, total, full = refs
    size = lo.shape[1]
    slots = pc.shape[1]
    d, first = lax.axis_index("depth"), lax.axis_index(("row", "col")) * rows
    zero = jnp.zeros((size, size), BF16)
    for i in range(rows):
        far = [(r, lo, lo_side, r, 1, r - REACH) for r in range(REACH) if r - REACH >= i - REACH]
        far += [(8 + r, hi, hi_side, r, -1, rows + r) for r in range(REACH) if rows + r <= i + REACH]
        lefts = []
        for *_, j in far:
            column = lax.rem(first + j + all_rows, all_rows)
            left = zero
            for k in range(4):
                here = (tab_a, tab_b)[k // 2][8 * (k % 2) + i, 0] == column
                left = jnp.where(here, x_row(xs, k, i), left)
            lefts.append(left)
        for p in range(slots):
            want = pc[i, p]
            acc = total[i * slots + p]
            for left, (at, straight, side, r, way, _) in zip(lefts, far):
                pick, found = jnp.int32(0), jnp.bool_(False)
                for m in range(slots):
                    match = tab_h[at, m] == want
                    pick = jnp.where(match, m, pick)
                    found = found | match
                n = lax.rem(way * (pick - d) + slots, slots)
                spot = (r * (slots - 1) + jnp.minimum(n, slots - 2)) * size
                block = jnp.where(
                    n < slots - 1,
                    straight[pl.ds(pl.multiple_of(spot, size), size), :],
                    side[r * size : r * size + size, :],
                )
                acc += jnp.dot(left, jnp.where(found, block, zero), preferred_element_type=F32)
            full[i * slots + p] = acc.astype(BF16)


def far_terms(scalars, xs, edges, total, all_rows):
    rows, slots = scalars[0].shape
    size = total.shape[-1]
    return pl.pallas_call(
        functools.partial(far_kernel, rows, all_rows),
        in_specs=[SMEM] * 4 + [VMEM] * 13,
        out_specs=VMEM,
        out_shape=pltpu.VMEM((rows * slots, size, size), BF16),
        cost_estimate=pl.CostEstimate(
            flops=2 * 24 * size**3, bytes_accessed=9 << 20, transcendentals=0
        ),
        compiler_params=pltpu.CompilerParams(vmem_limit_bytes=8 << 20),
        name="far_terms",
    )(*scalars, *[vmem(x) for x in (*xs, *edges, total)])


def q_kernel(rows, all_rows, pc, qc, lo_a, own_a, hi_a, lo_b, own_b, hi_b, full, s0, s1, s2, s3, mine, tiles, tabv, tab, res, sem, sems):
    size = full.shape[1]
    body = rows * size
    slots = pc.shape[1]
    raw = ((lo_a, lo_b), (own_a, own_b), (hi_a, hi_b))
    d, first = lax.axis_index("depth"), lax.axis_index(("row", "col")) * rows
    outward = copies([(full.at[i * slots + d], mine.at[i]) for i in range(rows)], sems)
    lane = lax.broadcasted_iota(I32, (8, 128), 1) % 64 // 8
    table = jnp.zeros((8, 128), F32)
    for n in range(3):
        for t in range(2):
            table = jnp.where(lane == 2 * n + t, raw[n][t][body : body + 8, :].astype(F32), table)
    tabv[...] = table.astype(I32)
    move = pltpu.make_async_copy(tabv, tab, sem)
    move.start()
    empty = 12 * slots * size
    tiles[pl.ds(empty, size), :] = jnp.zeros((size, 128), BF16)
    for n in range(3):
        for r in range(rows):
            for t in range(2):
                tile = raw[n][t][r * size : r * size + size, :]
                base = (((n * rows + r) * 2 + t) * 2) * size
                tiles[base : base + size, :] = tile
                tiles[base + size : base + 2 * size, :] = swapped(tile)
    move.wait()
    mask = low_half((size, 128))

    for i in range(rows):
        acc = jnp.zeros((size, size), F32)
        for p in range(slots):
            j = lax.rem(pc[i, p] - first + rows + all_rows, all_rows)
            picks = []
            for q in range(slots):
                half = (q + i) % 2
                pick = jnp.int32(empty)
                for m in range(slots):
                    spot = (j * 4 + (m // 2) * 2 + (m % 2 != half)) * size
                    column = tab[j % rows, 64 * (m % 2) + 8 * (2 * (j // rows) + m // 2)]
                    pick = jnp.where(column == qc[i, q], spot, pick)
                picks.append(tiles[pl.ds(pl.multiple_of(pick, size), size), :])
            pairs = [(picks[0], picks[1]), (picks[2], picks[3])]
            if i % 2:
                pairs = [(b, a) for a, b in pairs]
            right = jnp.concatenate([jnp.where(mask, a, b) for a, b in pairs], axis=1)
            acc += jnp.dot(full[i * slots + p], right, preferred_element_type=F32)
        value = acc.astype(BF16)
        res[2 * i] = value[:, :128]
        res[2 * i + 1] = value[:, 128:]
    for o, out in enumerate((s0, s1, s2, s3)):
        q = lax.rem(d + o, 4)
        even = mask == (q % 2 == 0)
        for e in range(rows // 2):
            out[e * size : e * size + size, :] = jnp.where(
                even, res[4 * e + q // 2], res[4 * e + 2 + q // 2]
            )
    for copy in outward:
        copy.wait()


def q_product(pc, qc, pieces, full, all_rows):
    rows, slots = pc.shape
    size = full.shape[1]
    return pl.pallas_call(
        functools.partial(q_kernel, rows, all_rows),
        in_specs=[SMEM] * 2 + [VMEM] * 7,
        out_specs=[VMEM] * 4 + [HBM],
        out_shape=[pltpu.VMEM((rows // 2 * size, 128), BF16)] * 4
        + [jax.ShapeDtypeStruct((rows, size, size), BF16)],
        scratch_shapes=[
            pltpu.VMEM(((12 * slots + 1) * size, 128), BF16),
            pltpu.VMEM((8, 128), I32),
            pltpu.SMEM((8, 128), I32),
            pltpu.VMEM((2 * rows, size, 128), BF16),
            pltpu.SemaphoreType.DMA,
            pltpu.SemaphoreType.DMA((rows,)),
        ],
        cost_estimate=pl.CostEstimate(
            flops=2 * rows * slots * size**3, bytes_accessed=5 << 20, transcendentals=0
        ),
        compiler_params=pltpu.CompilerParams(vmem_limit_bytes=24 << 20),
        name="q_product",
    )(pc, qc, *[vmem(x) for x in (*pieces, full)])


def join_kernel(t0, t1, t2, t3, out, held):
    size, d = out.shape[1], lax.axis_index("depth")
    for o, t in enumerate((t0, t1, t2, t3)):
        held[lax.rem(d - o + 4, 4)] = t[...]
    mask = low_half((size, 128))
    for side in range(2):

        @pl.when(d % 2 == side)
        def _():
            for i in range(out.shape[0]):
                rows = slice(i // 2 * size, i // 2 * size + size)
                for t in range(2):
                    a, b = held[2 * t, rows], held[2 * t + 1, rows]
                    if (side + i) % 2 == 0:
                        b = swapped(b)
                    else:
                        a = swapped(a)
                    out[i, :, 128 * t : 128 * t + 128] = jnp.where(mask, a, b)


def join(parts, rows, size):
    return pl.pallas_call(
        join_kernel,
        in_specs=[VMEM] * 4,
        out_specs=VMEM,
        out_shape=jax.ShapeDtypeStruct((rows, size, size), BF16),
        scratch_shapes=[pltpu.VMEM((4, *parts[0].shape), BF16)],
        compiler_params=pltpu.CompilerParams(vmem_limit_bytes=8 << 20),
        name="join",
    )(*[vmem(x) for x in parts])


def local(x_blocks, x_columns, h_blocks, h_columns, p_columns, q_columns):
    rows, _, size, _ = x_blocks.shape
    groups = lax.axis_size(("row", "col"))
    depth = lax.axis_size("depth")
    all_rows = rows * groups
    up = [(g, (g + 1) % groups) for g in range(groups)]
    down = [(b, a) for a, b in up]

    def turn(x, o):
        return lax.ppermute(x, "depth", [(s, (s + o) % depth) for s in range(depth)])

    def shift(x, pairs):
        return lax.ppermute(x, ("row", "col"), pairs)

    x_low, x_high, h_up, h_down = pack(x_blocks, x_columns, h_blocks, h_columns)
    h_lo, h_hi = shift(h_up, up), shift(h_down, down)
    low_one, high_three = turn(x_low, 1), turn(x_high, 3)
    high_one, low_three = turn(x_high, 1), turn(x_low, 3)
    low_two, high_two = turn(low_one, 1), turn(high_three, 3)
    xs = [x_low, x_high, low_one, high_one, low_three, high_three, low_two, high_two]

    h = h_blocks.reshape(-1, size)
    tables = (p_columns, h_columns)
    own = near_terms(own_kernel, (*tables, x_columns.T), (x_low, x_high, h), all_rows)
    a, tab_a = column_slices(xs[:4])
    a_lo, a_hi = shift(a, up), shift(a, down)
    send_lo, send_hi, tab_h = first_slots(h_lo, h_hi)
    edges = [h_lo, h_hi, turn(send_lo, 1), turn(send_hi, 3)]
    b, tab_b = column_slices(xs[4:])
    b_lo, b_hi = shift(b, up), shift(b, down)
    total = near_terms(near_kernel, (*tables, tab_a, tab_b), (*xs[2:], h, own), all_rows)
    full = far_terms((p_columns, tab_a, tab_b, tab_h), xs, edges, total, all_rows)
    pieces = (a_lo, a, a_hi, b_lo, b, b_hi)
    *parts, mine = q_product(p_columns, q_columns, pieces, full, all_rows)
    parts = [parts[0]] + [turn(parts[o], o) for o in range(1, depth)]
    product_q = join(parts, rows, size)
    return mine[:, None], product_q[:, None]


def solution(mesh):
    in_specs = (
        P(("row", "col"), "depth", None, None),
        P(("row", "col"), "depth"),
        P(("row", "col"), None, None, None),
        P(("row", "col"), None),
        P(("row", "col"), None),
        P(("row", "col"), None),
    )
    out_specs = (P(("row", "col"), "depth", None, None), P(("row", "col"), "depth", None, None))
    return jax.shard_map(local, mesh=mesh, in_specs=in_specs, out_specs=out_specs, check_vma=False)
```

```python
import functools

import jax
import jax.numpy as jnp
from jax import lax
from jax.experimental import pallas as pl
from jax.experimental.pallas import tpu as pltpu
from jax.sharding import PartitionSpec as P


REACH = 2
PAD = 16
BF16, F32, I32 = jnp.bfloat16, jnp.float32, jnp.int32


ANY = pl.BlockSpec(memory_space=pl.ANY)
SMEM = pl.BlockSpec(memory_space=pltpu.SMEM)
VMEM = pl.BlockSpec(memory_space=pltpu.VMEM)
HBM = pl.BlockSpec(memory_space=pltpu.HBM)


def low_half(shape):
    return lax.broadcasted_iota(I32, shape, 1) < 64


def swapped(tile):
    return pltpu.roll(tile.astype(F32), 64, 1).astype(tile.dtype)


def vmem(x):
    return pltpu.with_memory_space_constraint(x, pltpu.VMEM)


def hbm(x):
    return pltpu.with_memory_space_constraint(x, pltpu.HBM)


def copies(pairs, sems):
    made = [pltpu.make_async_copy(a, b, sems.at[n]) for n, (a, b) in enumerate(pairs)]
    for copy in made:
        copy.start()
    return made


def pack_kernel(x_columns, h_columns, x, h, x_low, x_high, h_up, h_down, xc, hc, sems):
    cut, size = x_low.shape
    tail = x_high.shape[0] - PAD
    edge = h_up.shape[0] - PAD
    rows, slots = hc.shape
    d, straight = lax.axis_index("depth"), slots - 1
    small = copies([(x_columns, xc), (h_columns, hc)], sems.at[pl.ds(14, 2)])
    moves = copies(
        [
            (x.at[pl.ds(0, cut)], x_low),
            (x.at[pl.ds(cut, tail)], x_high.at[pl.ds(0, tail)]),
        ]
        + [
            (
                h.at[pl.ds(pl.multiple_of(((start + r) * slots + lax.rem(d + way * n + slots, slots)) * size, size), size)],
                out.at[pl.ds((r * straight + n) * size, size)],
            )
            for out, start, way in ((h_up, rows - REACH, 1), (h_down, 0, -1))
            for r in range(REACH)
            for n in range(straight)
        ],
        sems,
    )
    shape = (PAD, size)
    row, lane = lax.broadcasted_iota(I32, shape, 0), lax.broadcasted_iota(I32, shape, 1)
    for move in small:
        move.wait()
    table = jnp.zeros(shape, I32)
    for r in range(rows):
        table = jnp.where(row == r, xc[0, r], table)
    x_high[tail:, :] = table.astype(F32).astype(BF16)
    for out, start in ((h_up, rows - REACH), (h_down, 0)):
        table = jnp.zeros(shape, I32)
        for r in range(REACH):
            for m in range(slots):
                table = jnp.where((row == r) & (lane == m), hc[start + r, m], table)
        out[edge:, :] = table.astype(F32).astype(BF16)
    for move in moves:
        move.wait()


def pack(x_blocks, x_columns, h_blocks, h_columns):
    rows, slots, size, _ = h_blocks.shape
    x, h = x_blocks.reshape(-1, size), h_blocks.reshape(-1, size)
    half = rows // 2 * size
    edge = pltpu.VMEM((REACH * (slots - 1) * size + PAD, size), BF16)
    return pl.pallas_call(
        pack_kernel,
        in_specs=[HBM] * 4,
        out_specs=[VMEM] * 4,
        out_shape=[
            pltpu.VMEM((half, size), BF16),
            pltpu.VMEM((x.shape[0] - half + PAD, size), BF16),
            edge,
            edge,
        ],
        scratch_shapes=[
            pltpu.SMEM((1, rows), I32),
            pltpu.SMEM((rows, slots), I32),
            pltpu.SemaphoreType.DMA((16,)),
        ],
        compiler_params=pltpu.CompilerParams(vmem_limit_bytes=8 << 20),
        name="pack",
    )(*[hbm(a) for a in (x_columns.T, h_columns, x, h)])


TABLE = pltpu.VMEM((16, 128), I32)


def whole(table, parts):
    for n, part in enumerate(parts):
        table[8 * n : 8 * n + 8, :] = part.astype(F32).astype(I32)


def slice_kernel(a_low, a_high, b_low, b_high, out, table):
    d = lax.axis_index("depth")
    tile = pl.ds(pl.multiple_of(d // 2 * 128, 128), 128)
    cut = a_low.shape[0]
    whole(table, [x[x.shape[0] - PAD : x.shape[0] - PAD + 8, :128] for x in (a_high, b_high)])
    for upper in range(2):

        @pl.when(d % 2 == upper)
        def _():
            for left, right, rows in ((a_low, b_low, slice(0, cut)), (a_high, b_high, slice(cut, None))):
                a, b = left[:, tile], right[:, tile]
                a, b = (swapped(a), b) if upper else (a, swapped(b))
                out[rows, :] = jnp.where(low_half(a.shape), a, b)


def column_slices(payloads):
    low, high = payloads[:2]
    return pl.pallas_call(
        slice_kernel,
        in_specs=[VMEM] * 4,
        out_specs=[VMEM, VMEM],
        out_shape=[pltpu.VMEM((low.shape[0] + high.shape[0], 128), BF16), TABLE],
        compiler_params=pltpu.CompilerParams(vmem_limit_bytes=8 << 20),
        name="column_slices",
    )(*[vmem(x) for x in payloads])


def first_slot_kernel(lo, hi, out_lo, out_hi, table):
    size = lo.shape[1]
    whole(table, [x[x.shape[0] - PAD : x.shape[0] - PAD + 8, :128] for x in (lo, hi)])
    step = (lo.shape[0] - PAD) // REACH
    for source, out in ((lo, out_lo), (hi, out_hi)):
        for r in range(REACH):
            out[r * size : r * size + size, :] = source[r * step : r * step + size, :]


def first_slots(lo, hi):
    size = lo.shape[1]
    return pl.pallas_call(
        first_slot_kernel,
        in_specs=[VMEM] * 2,
        out_specs=[VMEM] * 3,
        out_shape=[pltpu.VMEM((REACH * size, size), BF16)] * 2 + [TABLE],
        compiler_params=pltpu.CompilerParams(vmem_limit_bytes=4 << 20),
        name="first_slots",
    )(vmem(lo), vmem(hi))


def x_row(xs, k, i):
    cut, size = xs[0].shape
    at = i * size % cut
    return xs[2 * k + i * size // cut][at : at + size, :]


def own_block(column, first, all_rows, want, hc, h, zero):
    rows, slots = hc.shape
    size = h.shape[1]
    j = lax.rem(column - first + all_rows, all_rows)
    row = jnp.minimum(j, rows - 1)
    pick, found = jnp.int32(0), jnp.bool_(False)
    for m in range(slots):
        match = (hc[row, m] == want) & (j < rows)
        pick = jnp.where(match, m, pick)
        found = found | match
    spot = pl.multiple_of((row * slots + pick) * size, size)
    return jnp.where(found, h[pl.ds(spot, size), :], zero)


def own_kernel(rows, all_rows, pc, hc, xc, low, high, h, total):
    size = h.shape[1]
    slots = pc.shape[1]
    first = lax.axis_index(("row", "col")) * rows
    zero = jnp.zeros((size, size), BF16)
    for i in range(rows):
        for p in range(slots):
            block = own_block(xc[0, i], first, all_rows, pc[i, p], hc, h, zero)
            total[i * slots + p] = jnp.dot(x_row((low, high), 0, i), block, preferred_element_type=F32)


def near_kernel(rows, all_rows, pc, hc, tab_a, tab_b, *refs):
    *xs, h, before, total = refs
    size = h.shape[1]
    slots = pc.shape[1]
    first = lax.axis_index(("row", "col")) * rows
    zero = jnp.zeros((size, size), BF16)
    for i in range(rows):
        for p in range(slots):
            acc = before[i * slots + p]
            for k in range(1, 4):
                column = (tab_a, tab_b)[k // 2][8 * (k % 2) + i, 0]
                block = own_block(column, first, all_rows, pc[i, p], hc, h, zero)
                acc += jnp.dot(x_row(xs, k - 1, i), block, preferred_element_type=F32)
            total[i * slots + p] = acc


def near_terms(kernel, scalars, arrays, all_rows):
    rows, slots = scalars[0].shape
    size = arrays[0].shape[1]
    terms = 3 if len(arrays) > 3 else 1
    return pl.pallas_call(
        functools.partial(kernel, rows, all_rows),
        in_specs=[SMEM] * len(scalars) + [VMEM] * len(arrays),
        out_specs=VMEM,
        out_shape=pltpu.VMEM((rows * slots, size, size), F32),
        cost_estimate=pl.CostEstimate(
            flops=2 * rows * slots * terms * size**3, bytes_accessed=9 << 20, transcendentals=0
        ),
        compiler_params=pltpu.CompilerParams(vmem_limit_bytes=8 << 20),
    )(*scalars, *[vmem(x) for x in arrays])


def far_kernel(rows, all_rows, pc, tab_a, tab_b, tab_h, *refs):
    *xs, lo, hi, lo_side, hi_side, total, full = refs
    size = lo.shape[1]
    slots = pc.shape[1]
    d, first = lax.axis_index("depth"), lax.axis_index(("row", "col")) * rows
    zero = jnp.zeros((size, size), BF16)
    for i in range(rows):
        far = [(r, lo, lo_side, r, 1, r - REACH) for r in range(REACH) if r - REACH >= i - REACH]
        far += [(8 + r, hi, hi_side, r, -1, rows + r) for r in range(REACH) if rows + r <= i + REACH]
        lefts = []
        for *_, j in far:
            column = lax.rem(first + j + all_rows, all_rows)
            left = zero
            for k in range(4):
                here = (tab_a, tab_b)[k // 2][8 * (k % 2) + i, 0] == column
                left = jnp.where(here, x_row(xs, k, i), left)
            lefts.append(left)
        for p in range(slots):
            want = pc[i, p]
            acc = total[i * slots + p]
            for left, (at, straight, side, r, way, _) in zip(lefts, far):
                pick, found = jnp.int32(0), jnp.bool_(False)
                for m in range(slots):
                    match = tab_h[at, m] == want
                    pick = jnp.where(match, m, pick)
                    found = found | match
                n = lax.rem(way * (pick - d) + slots, slots)
                spot = (r * (slots - 1) + jnp.minimum(n, slots - 2)) * size
                block = jnp.where(
                    n < slots - 1,
                    straight[pl.ds(pl.multiple_of(spot, size), size), :],
                    side[r * size : r * size + size, :],
                )
                acc += jnp.dot(left, jnp.where(found, block, zero), preferred_element_type=F32)
            full[i * slots + p] = acc.astype(BF16)


def far_terms(scalars, xs, edges, total, all_rows):
    rows, slots = scalars[0].shape
    size = total.shape[-1]
    return pl.pallas_call(
        functools.partial(far_kernel, rows, all_rows),
        in_specs=[SMEM] * 4 + [VMEM] * 13,
        out_specs=VMEM,
        out_shape=pltpu.VMEM((rows * slots, size, size), BF16),
        cost_estimate=pl.CostEstimate(
            flops=2 * 24 * size**3, bytes_accessed=9 << 20, transcendentals=0
        ),
        compiler_params=pltpu.CompilerParams(vmem_limit_bytes=8 << 20),
        name="far_terms",
    )(*scalars, *[vmem(x) for x in (*xs, *edges, total)])


def q_kernel(rows, all_rows, pc, qc, lo_a, own_a, hi_a, lo_b, own_b, hi_b, full, s0, s1, s2, s3, mine, tiles, tabv, tab, res, sem, sems):
    size = full.shape[1]
    body = rows * size
    slots = pc.shape[1]
    raw = ((lo_a, lo_b), (own_a, own_b), (hi_a, hi_b))
    d, first = lax.axis_index("depth"), lax.axis_index(("row", "col")) * rows
    outward = copies([(full.at[i * slots + d], mine.at[i]) for i in range(rows)], sems)
    lane = lax.broadcasted_iota(I32, (8, 128), 1) % 64 // 8
    table = jnp.zeros((8, 128), F32)
    for n in range(3):
        for t in range(2):
            table = jnp.where(lane == 2 * n + t, raw[n][t][body : body + 8, :].astype(F32), table)
    tabv[...] = table.astype(I32)
    move = pltpu.make_async_copy(tabv, tab, sem)
    move.start()
    empty = 12 * slots * size
    tiles[pl.ds(empty, size), :] = jnp.zeros((size, 128), BF16)
    for n in range(3):
        for r in range(rows):
            for t in range(2):
                tile = raw[n][t][r * size : r * size + size, :]
                base = (((n * rows + r) * 2 + t) * 2) * size
                tiles[base : base + size, :] = tile
                tiles[base + size : base + 2 * size, :] = swapped(tile)
    move.wait()
    mask = low_half((size, 128))

    for i in range(rows):
        acc = jnp.zeros((size, size), F32)
        for p in range(slots):
            j = lax.rem(pc[i, p] - first + rows + all_rows, all_rows)
            picks = []
            for q in range(slots):
                half = (q + i) % 2
                pick = jnp.int32(empty)
                for m in range(slots):
                    spot = (j * 4 + (m // 2) * 2 + (m % 2 != half)) * size
                    column = tab[j % rows, 64 * (m % 2) + 8 * (2 * (j // rows) + m // 2)]
                    pick = jnp.where(column == qc[i, q], spot, pick)
                picks.append(tiles[pl.ds(pl.multiple_of(pick, size), size), :])
            pairs = [(picks[0], picks[1]), (picks[2], picks[3])]
            if i % 2:
                pairs = [(b, a) for a, b in pairs]
            right = jnp.concatenate([jnp.where(mask, a, b) for a, b in pairs], axis=1)
            acc += jnp.dot(full[i * slots + p], right, preferred_element_type=F32)
        value = acc.astype(BF16)
        res[2 * i] = value[:, :128]
        res[2 * i + 1] = value[:, 128:]
    for o, out in enumerate((s0, s1, s2, s3)):
        q = lax.rem(d + o, 4)
        even = mask == (q % 2 == 0)
        for e in range(rows // 2):
            out[e * size : e * size + size, :] = jnp.where(
                even, res[4 * e + q // 2], res[4 * e + 2 + q // 2]
            )
    for copy in outward:
        copy.wait()


def q_product(pc, qc, pieces, full, all_rows):
    rows, slots = pc.shape
    size = full.shape[1]
    return pl.pallas_call(
        functools.partial(q_kernel, rows, all_rows),
        in_specs=[SMEM] * 2 + [VMEM] * 7,
        out_specs=[VMEM] * 4 + [HBM],
        out_shape=[pltpu.VMEM((rows // 2 * size, 128), BF16)] * 4
        + [jax.ShapeDtypeStruct((rows, size, size), BF16)],
        scratch_shapes=[
            pltpu.VMEM(((12 * slots + 1) * size, 128), BF16),
            pltpu.VMEM((8, 128), I32),
            pltpu.SMEM((8, 128), I32),
            pltpu.VMEM((2 * rows, size, 128), BF16),
            pltpu.SemaphoreType.DMA,
            pltpu.SemaphoreType.DMA((rows,)),
        ],
        cost_estimate=pl.CostEstimate(
            flops=2 * rows * slots * size**3, bytes_accessed=5 << 20, transcendentals=0
        ),
        compiler_params=pltpu.CompilerParams(vmem_limit_bytes=24 << 20),
        name="q_product",
    )(pc, qc, *[vmem(x) for x in (*pieces, full)])


def join_kernel(t0, t1, t2, t3, out, held, ready, sems):
    size, d = out.shape[1], lax.axis_index("depth")
    for o, t in enumerate((t0, t1, t2, t3)):
        held[lax.rem(d - o + 4, 4)] = t[...]
    mask = low_half((size, 128))
    for side in range(2):

        @pl.when(d % 2 == side)
        def _():
            for i in range(out.shape[0]):
                rows = slice(i // 2 * size, i // 2 * size + size)
                for t in range(2):
                    a, b = held[2 * t, rows], held[2 * t + 1, rows]
                    if (side + i) % 2 == 0:
                        b = swapped(b)
                    else:
                        a = swapped(a)
                    ready[i, :, 128 * t : 128 * t + 128] = jnp.where(mask, a, b)
                pltpu.make_async_copy(ready.at[i], out.at[i], sems.at[i]).start()
    for i in range(out.shape[0]):
        pltpu.make_async_copy(ready.at[i], out.at[i], sems.at[i]).wait()


def join(parts, rows, size):
    return pl.pallas_call(
        join_kernel,
        in_specs=[VMEM] * 4,
        out_specs=HBM,
        out_shape=jax.ShapeDtypeStruct((rows, size, size), BF16),
        scratch_shapes=[
            pltpu.VMEM((4, *parts[0].shape), BF16),
            pltpu.VMEM((rows, size, size), BF16),
            pltpu.SemaphoreType.DMA((rows,)),
        ],
        compiler_params=pltpu.CompilerParams(vmem_limit_bytes=8 << 20),
        name="join",
    )(*[vmem(x) for x in parts])


def local(x_blocks, x_columns, h_blocks, h_columns, p_columns, q_columns):
    rows, _, size, _ = x_blocks.shape
    groups = lax.axis_size(("row", "col"))
    depth = lax.axis_size("depth")
    all_rows = rows * groups
    up = [(g, (g + 1) % groups) for g in range(groups)]
    down = [(b, a) for a, b in up]

    def turn(x, o):
        return lax.ppermute(x, "depth", [(s, (s + o) % depth) for s in range(depth)])

    def shift(x, pairs):
        return lax.ppermute(x, ("row", "col"), pairs)

    x_low, x_high, h_up, h_down = pack(x_blocks, x_columns, h_blocks, h_columns)
    h_lo, h_hi = shift(h_up, up), shift(h_down, down)
    low_one, high_three = turn(x_low, 1), turn(x_high, 3)
    high_one, low_three = turn(x_high, 1), turn(x_low, 3)
    low_two, high_two = turn(low_one, 1), turn(high_three, 3)
    xs = [x_low, x_high, low_one, high_one, low_three, high_three, low_two, high_two]

    h = h_blocks.reshape(-1, size)
    tables = (p_columns, h_columns)
    own = near_terms(own_kernel, (*tables, x_columns.T), (x_low, x_high, h), all_rows)
    a, tab_a = column_slices(xs[:4])
    a_lo, a_hi = shift(a, up), shift(a, down)
    send_lo, send_hi, tab_h = first_slots(h_lo, h_hi)
    edges = [h_lo, h_hi, turn(send_lo, 1), turn(send_hi, 3)]
    b, tab_b = column_slices(xs[4:])
    b_lo, b_hi = shift(b, up), shift(b, down)
    total = near_terms(near_kernel, (*tables, tab_a, tab_b), (*xs[2:], h, own), all_rows)
    full = far_terms((p_columns, tab_a, tab_b, tab_h), xs, edges, total, all_rows)
    pieces = (a_lo, a, a_hi, b_lo, b, b_hi)
    *parts, mine = q_product(p_columns, q_columns, pieces, full, all_rows)
    parts = [parts[0]] + [turn(parts[o], o) for o in range(1, depth)]
    product_q = join(parts, rows, size)
    return mine[:, None], product_q[:, None]


def solution(mesh):
    in_specs = (
        P(("row", "col"), "depth", None, None),
        P(("row", "col"), "depth"),
        P(("row", "col"), None, None, None),
        P(("row", "col"), None),
        P(("row", "col"), None),
        P(("row", "col"), None),
    )
    out_specs = (P(("row", "col"), "depth", None, None), P(("row", "col"), "depth", None, None))
    return jax.shard_map(local, mesh=mesh, in_specs=in_specs, out_specs=out_specs, check_vma=False)
```

```python
import functools

import jax
import jax.numpy as jnp
from jax import lax
from jax.experimental import pallas as pl
from jax.experimental.pallas import tpu as pltpu
from jax.sharding import PartitionSpec as P


REACH = 2
PAD = 16
BF16, F32, I32 = jnp.bfloat16, jnp.float32, jnp.int32


ANY = pl.BlockSpec(memory_space=pl.ANY)
SMEM = pl.BlockSpec(memory_space=pltpu.SMEM)
VMEM = pl.BlockSpec(memory_space=pltpu.VMEM)
HBM = pl.BlockSpec(memory_space=pltpu.HBM)


def low_half(shape):
    return lax.broadcasted_iota(I32, shape, 1) < 64


def swapped(tile):
    return pltpu.roll(tile.astype(F32), 64, 1).astype(tile.dtype)


def vmem(x):
    return pltpu.with_memory_space_constraint(x, pltpu.VMEM)


def hbm(x):
    return pltpu.with_memory_space_constraint(x, pltpu.HBM)


def copies(pairs, sems):
    made = [pltpu.make_async_copy(a, b, sems.at[n]) for n, (a, b) in enumerate(pairs)]
    for copy in made:
        copy.start()
    return made


def pack_kernel(x_columns, h_columns, x, h, x_low, x_high, h_up, h_down, xc, hc, sems):
    cut, size = x_low.shape
    tail = x_high.shape[0] - PAD
    edge = h_up.shape[0] - PAD
    rows, slots = hc.shape
    d, straight = lax.axis_index("depth"), slots - 1
    small = copies([(x_columns, xc), (h_columns, hc)], sems.at[pl.ds(14, 2)])
    moves = copies(
        [
            (x.at[pl.ds(0, cut)], x_low),
            (x.at[pl.ds(cut, tail)], x_high.at[pl.ds(0, tail)]),
        ]
        + [
            (
                h.at[pl.ds(pl.multiple_of(((start + r) * slots + lax.rem(d + way * n + slots, slots)) * size, size), size)],
                out.at[pl.ds((r * straight + n) * size, size)],
            )
            for out, start, way in ((h_up, rows - REACH, 1), (h_down, 0, -1))
            for r in range(REACH)
            for n in range(straight)
        ],
        sems,
    )
    shape = (PAD, size)
    row, lane = lax.broadcasted_iota(I32, shape, 0), lax.broadcasted_iota(I32, shape, 1)
    for move in small:
        move.wait()
    table = jnp.zeros(shape, I32)
    for r in range(rows):
        table = jnp.where(row == r, xc[0, r], table)
    x_high[tail:, :] = table.astype(F32).astype(BF16)
    for out, start, base in ((h_up, rows - REACH, 0), (h_down, 0, REACH)):
        table = jnp.zeros(shape, I32)
        for r in range(REACH):
            for m in range(slots):
                table = jnp.where((row == base + r) & (lane == m), hc[start + r, m], table)
        out[edge:, :] = table.astype(F32).astype(BF16)
    for move in moves:
        move.wait()


def pack(x_blocks, x_columns, h_blocks, h_columns):
    rows, slots, size, _ = h_blocks.shape
    x, h = x_blocks.reshape(-1, size), h_blocks.reshape(-1, size)
    half = rows // 2 * size
    edge = pltpu.VMEM((REACH * (slots - 1) * size + PAD, size), BF16)
    return pl.pallas_call(
        pack_kernel,
        in_specs=[HBM] * 4,
        out_specs=[VMEM] * 4,
        out_shape=[
            pltpu.VMEM((half, size), BF16),
            pltpu.VMEM((x.shape[0] - half + PAD, size), BF16),
            edge,
            edge,
        ],
        scratch_shapes=[
            pltpu.SMEM((1, rows), I32),
            pltpu.SMEM((rows, slots), I32),
            pltpu.SemaphoreType.DMA((16,)),
        ],
        compiler_params=pltpu.CompilerParams(vmem_limit_bytes=8 << 20),
        name="pack",
    )(*[hbm(a) for a in (x_columns.T, h_columns, x, h)])


TABLE = pltpu.VMEM((8, 128), I32)


def tail(x):
    return x[x.shape[0] - PAD : x.shape[0] - PAD + 8, :128].astype(F32)


def slice_kernel(a_low, a_high, b_low, b_high, out, table):
    d = lax.axis_index("depth")
    tile = pl.ds(pl.multiple_of(d // 2 * 128, 128), 128)
    cut = a_low.shape[0]
    table[...] = jnp.where(low_half((8, 128)), tail(a_high), tail(b_high)).astype(I32)
    for upper in range(2):

        @pl.when(d % 2 == upper)
        def _():
            for left, right, rows in ((a_low, b_low, slice(0, cut)), (a_high, b_high, slice(cut, None))):
                a, b = left[:, tile], right[:, tile]
                a, b = (swapped(a), b) if upper else (a, swapped(b))
                out[rows, :] = jnp.where(low_half(a.shape), a, b)


def column_slices(payloads):
    low, high = payloads[:2]
    return pl.pallas_call(
        slice_kernel,
        in_specs=[VMEM] * 4,
        out_specs=[VMEM, VMEM],
        out_shape=[pltpu.VMEM((low.shape[0] + high.shape[0], 128), BF16), TABLE],
        compiler_params=pltpu.CompilerParams(vmem_limit_bytes=8 << 20),
        name="column_slices",
    )(*[vmem(x) for x in payloads])


def first_slot_kernel(lo, hi, out_lo, out_hi, table):
    size = lo.shape[1]
    table[...] = (tail(lo) + tail(hi)).astype(I32)
    step = (lo.shape[0] - PAD) // REACH
    for source, out in ((lo, out_lo), (hi, out_hi)):
        for r in range(REACH):
            out[r * size : r * size + size, :] = source[r * step : r * step + size, :]


def first_slots(lo, hi):
    size = lo.shape[1]
    return pl.pallas_call(
        first_slot_kernel,
        in_specs=[VMEM] * 2,
        out_specs=[VMEM] * 3,
        out_shape=[pltpu.VMEM((REACH * size, size), BF16)] * 2 + [TABLE],
        compiler_params=pltpu.CompilerParams(vmem_limit_bytes=4 << 20),
        name="first_slots",
    )(vmem(lo), vmem(hi))


def x_row(xs, k, i):
    cut, size = xs[0].shape
    at = i * size % cut
    return xs[2 * k + i * size // cut][at : at + size, :]


def own_block(column, first, all_rows, want, hc, h, zero):
    rows, slots = hc.shape
    size = h.shape[1]
    j = lax.rem(column - first + all_rows, all_rows)
    row = jnp.minimum(j, rows - 1)
    pick, found = jnp.int32(0), jnp.bool_(False)
    for m in range(slots):
        match = (hc[row, m] == want) & (j < rows)
        pick = jnp.where(match, m, pick)
        found = found | match
    spot = pl.multiple_of((row * slots + pick) * size, size)
    return jnp.where(found, h[pl.ds(spot, size), :], zero)


def own_kernel(rows, all_rows, pc, hc, xc, low, high, h, total):
    size = h.shape[1]
    slots = pc.shape[1]
    first = lax.axis_index(("row", "col")) * rows
    zero = jnp.zeros((size, size), BF16)
    for i in range(rows):
        for p in range(slots):
            block = own_block(xc[0, i], first, all_rows, pc[i, p], hc, h, zero)
            total[i * slots + p] = jnp.dot(x_row((low, high), 0, i), block, preferred_element_type=F32)


def near_kernel(rows, all_rows, pc, hc, tab_a, tab_b, *refs):
    *xs, h, before, total = refs
    size = h.shape[1]
    slots = pc.shape[1]
    first = lax.axis_index(("row", "col")) * rows
    zero = jnp.zeros((size, size), BF16)
    for i in range(rows):
        for p in range(slots):
            acc = before[i * slots + p]
            for k in range(1, 4):
                column = (tab_a, tab_b)[k // 2][i, 64 * (k % 2)]
                block = own_block(column, first, all_rows, pc[i, p], hc, h, zero)
                acc += jnp.dot(x_row(xs, k - 1, i), block, preferred_element_type=F32)
            total[i * slots + p] = acc


def near_terms(kernel, scalars, arrays, all_rows):
    rows, slots = scalars[0].shape
    size = arrays[0].shape[1]
    terms = 3 if len(arrays) > 3 else 1
    return pl.pallas_call(
        functools.partial(kernel, rows, all_rows),
        in_specs=[SMEM] * len(scalars) + [VMEM] * len(arrays),
        out_specs=VMEM,
        out_shape=pltpu.VMEM((rows * slots, size, size), F32),
        cost_estimate=pl.CostEstimate(
            flops=2 * rows * slots * terms * size**3, bytes_accessed=9 << 20, transcendentals=0
        ),
        compiler_params=pltpu.CompilerParams(vmem_limit_bytes=8 << 20),
    )(*scalars, *[vmem(x) for x in arrays])


def far_kernel(rows, all_rows, pc, tab_a, tab_b, tab_h, *refs):
    *xs, lo, hi, lo_side, hi_side, total, full = refs
    size = lo.shape[1]
    slots = pc.shape[1]
    d, first = lax.axis_index("depth"), lax.axis_index(("row", "col")) * rows
    zero = jnp.zeros((size, size), BF16)
    for i in range(rows):
        far = [(r, lo, lo_side, r, 1, r - REACH) for r in range(REACH) if r - REACH >= i - REACH]
        far += [(REACH + r, hi, hi_side, r, -1, rows + r) for r in range(REACH) if rows + r <= i + REACH]
        lefts = []
        for *_, j in far:
            column = lax.rem(first + j + all_rows, all_rows)
            left = zero
            for k in range(4):
                here = (tab_a, tab_b)[k // 2][i, 64 * (k % 2)] == column
                left = jnp.where(here, x_row(xs, k, i), left)
            lefts.append(left)
        for p in range(slots):
            want = pc[i, p]
            acc = total[i * slots + p]
            for left, (at, straight, side, r, way, _) in zip(lefts, far):
                pick, found = jnp.int32(0), jnp.bool_(False)
                for m in range(slots):
                    match = tab_h[at, m] == want
                    pick = jnp.where(match, m, pick)
                    found = found | match
                n = lax.rem(way * (pick - d) + slots, slots)
                spot = (r * (slots - 1) + jnp.minimum(n, slots - 2)) * size
                block = jnp.where(
                    n < slots - 1,
                    straight[pl.ds(pl.multiple_of(spot, size), size), :],
                    side[r * size : r * size + size, :],
                )
                acc += jnp.dot(left, jnp.where(found, block, zero), preferred_element_type=F32)
            full[i * slots + p] = acc.astype(BF16)


def far_terms(scalars, xs, edges, total, all_rows):
    rows, slots = scalars[0].shape
    size = total.shape[-1]
    return pl.pallas_call(
        functools.partial(far_kernel, rows, all_rows),
        in_specs=[SMEM] * 4 + [VMEM] * 13,
        out_specs=VMEM,
        out_shape=pltpu.VMEM((rows * slots, size, size), BF16),
        cost_estimate=pl.CostEstimate(
            flops=2 * 24 * size**3, bytes_accessed=9 << 20, transcendentals=0
        ),
        compiler_params=pltpu.CompilerParams(vmem_limit_bytes=8 << 20),
        name="far_terms",
    )(*scalars, *[vmem(x) for x in (*xs, *edges, total)])


def q_kernel(rows, all_rows, pc, qc, lo_a, own_a, hi_a, lo_b, own_b, hi_b, full, s0, s1, s2, s3, mine, tiles, tabv, tab, res, sem, sems):
    size = full.shape[1]
    body = rows * size
    slots = pc.shape[1]
    raw = ((lo_a, lo_b), (own_a, own_b), (hi_a, hi_b))
    d, first = lax.axis_index("depth"), lax.axis_index(("row", "col")) * rows
    outward = copies([(full.at[i * slots + d], mine.at[i]) for i in range(rows)], sems)
    lane = lax.broadcasted_iota(I32, (8, 128), 1) % 64 // 8
    table = jnp.zeros((8, 128), F32)
    for n in range(3):
        for t in range(2):
            table = jnp.where(lane == 2 * n + t, raw[n][t][body : body + 8, :].astype(F32), table)
    tabv[...] = table.astype(I32)
    move = pltpu.make_async_copy(tabv, tab, sem)
    move.start()
    empty = 12 * slots * size
    tiles[pl.ds(empty, size), :] = jnp.zeros((size, 128), BF16)
    for n in range(3):
        for r in range(rows):
            for t in range(2):
                tile = raw[n][t][r * size : r * size + size, :]
                base = (((n * rows + r) * 2 + t) * 2) * size
                tiles[base : base + size, :] = tile
                tiles[base + size : base + 2 * size, :] = swapped(tile)
    move.wait()
    mask = low_half((size, 128))

    for i in range(rows):
        acc = jnp.zeros((size, size), F32)
        for p in range(slots):
            j = lax.rem(pc[i, p] - first + rows + all_rows, all_rows)
            picks = []
            for q in range(slots):
                half = (q + i) % 2
                pick = jnp.int32(empty)
                for m in range(slots):
                    spot = (j * 4 + (m // 2) * 2 + (m % 2 != half)) * size
                    column = tab[j % rows, 64 * (m % 2) + 8 * (2 * (j // rows) + m // 2)]
                    pick = jnp.where(column == qc[i, q], spot, pick)
                picks.append(tiles[pl.ds(pl.multiple_of(pick, size), size), :])
            pairs = [(picks[0], picks[1]), (picks[2], picks[3])]
            if i % 2:
                pairs = [(b, a) for a, b in pairs]
            right = jnp.concatenate([jnp.where(mask, a, b) for a, b in pairs], axis=1)
            acc += jnp.dot(full[i * slots + p], right, preferred_element_type=F32)
        value = acc.astype(BF16)
        res[2 * i] = value[:, :128]
        res[2 * i + 1] = value[:, 128:]
    for o, out in enumerate((s0, s1, s2, s3)):
        q = lax.rem(d + o, 4)
        even = mask == (q % 2 == 0)
        for e in range(rows // 2):
            out[e * size : e * size + size, :] = jnp.where(
                even, res[4 * e + q // 2], res[4 * e + 2 + q // 2]
            )
    for copy in outward:
        copy.wait()


def q_product(pc, qc, pieces, full, all_rows):
    rows, slots = pc.shape
    size = full.shape[1]
    return pl.pallas_call(
        functools.partial(q_kernel, rows, all_rows),
        in_specs=[SMEM] * 2 + [VMEM] * 7,
        out_specs=[VMEM] * 4 + [HBM],
        out_shape=[pltpu.VMEM((rows // 2 * size, 128), BF16)] * 4
        + [jax.ShapeDtypeStruct((rows, size, size), BF16)],
        scratch_shapes=[
            pltpu.VMEM(((12 * slots + 1) * size, 128), BF16),
            pltpu.VMEM((8, 128), I32),
            pltpu.SMEM((8, 128), I32),
            pltpu.VMEM((2 * rows, size, 128), BF16),
            pltpu.SemaphoreType.DMA,
            pltpu.SemaphoreType.DMA((rows,)),
        ],
        cost_estimate=pl.CostEstimate(
            flops=2 * rows * slots * size**3, bytes_accessed=5 << 20, transcendentals=0
        ),
        compiler_params=pltpu.CompilerParams(vmem_limit_bytes=24 << 20),
        name="q_product",
    )(pc, qc, *[vmem(x) for x in (*pieces, full)])


def join_kernel(t0, t1, t2, t3, out, held, ready, sems):
    size, d = out.shape[1], lax.axis_index("depth")
    for o, t in enumerate((t0, t1, t2, t3)):
        held[lax.rem(d - o + 4, 4)] = t[...]
    mask = low_half((size, 128))
    for side in range(2):

        @pl.when(d % 2 == side)
        def _():
            for i in range(out.shape[0]):
                rows = slice(i // 2 * size, i // 2 * size + size)
                for t in range(2):
                    a, b = held[2 * t, rows], held[2 * t + 1, rows]
                    if (side + i) % 2 == 0:
                        b = swapped(b)
                    else:
                        a = swapped(a)
                    ready[i, :, 128 * t : 128 * t + 128] = jnp.where(mask, a, b)
                pltpu.make_async_copy(ready.at[i], out.at[i], sems.at[i]).start()
    for i in range(out.shape[0]):
        pltpu.make_async_copy(ready.at[i], out.at[i], sems.at[i]).wait()


def join(parts, rows, size):
    return pl.pallas_call(
        join_kernel,
        in_specs=[VMEM] * 4,
        out_specs=HBM,
        out_shape=jax.ShapeDtypeStruct((rows, size, size), BF16),
        scratch_shapes=[
            pltpu.VMEM((4, *parts[0].shape), BF16),
            pltpu.VMEM((rows, size, size), BF16),
            pltpu.SemaphoreType.DMA((rows,)),
        ],
        compiler_params=pltpu.CompilerParams(vmem_limit_bytes=8 << 20),
        name="join",
    )(*[vmem(x) for x in parts])


def local(x_blocks, x_columns, h_blocks, h_columns, p_columns, q_columns):
    rows, _, size, _ = x_blocks.shape
    groups = lax.axis_size(("row", "col"))
    depth = lax.axis_size("depth")
    all_rows = rows * groups
    up = [(g, (g + 1) % groups) for g in range(groups)]
    down = [(b, a) for a, b in up]

    def turn(x, o):
        return lax.ppermute(x, "depth", [(s, (s + o) % depth) for s in range(depth)])

    def shift(x, pairs):
        return lax.ppermute(x, ("row", "col"), pairs)

    x_low, x_high, h_up, h_down = pack(x_blocks, x_columns, h_blocks, h_columns)
    h_lo, h_hi = shift(h_up, up), shift(h_down, down)
    low_one, high_three = turn(x_low, 1), turn(x_high, 3)
    high_one, low_three = turn(x_high, 1), turn(x_low, 3)
    low_two, high_two = turn(low_one, 1), turn(high_three, 3)
    xs = [x_low, x_high, low_one, high_one, low_three, high_three, low_two, high_two]

    h = h_blocks.reshape(-1, size)
    tables = (p_columns, h_columns)
    own = near_terms(own_kernel, (*tables, x_columns.T), (x_low, x_high, h), all_rows)
    a, tab_a = column_slices(xs[:4])
    a_lo, a_hi = shift(a, up), shift(a, down)
    send_lo, send_hi, tab_h = first_slots(h_lo, h_hi)
    edges = [h_lo, h_hi, turn(send_lo, 1), turn(send_hi, 3)]
    b, tab_b = column_slices(xs[4:])
    b_lo, b_hi = shift(b, up), shift(b, down)
    total = near_terms(near_kernel, (*tables, tab_a, tab_b), (*xs[2:], h, own), all_rows)
    full = far_terms((p_columns, tab_a, tab_b, tab_h), xs, edges, total, all_rows)
    pieces = (a_lo, a, a_hi, b_lo, b, b_hi)
    *parts, mine = q_product(p_columns, q_columns, pieces, full, all_rows)
    parts = [parts[0]] + [turn(parts[o], o) for o in range(1, depth)]
    product_q = join(parts, rows, size)
    return mine[:, None], product_q[:, None]


def solution(mesh):
    in_specs = (
        P(("row", "col"), "depth", None, None),
        P(("row", "col"), "depth"),
        P(("row", "col"), None, None, None),
        P(("row", "col"), None),
        P(("row", "col"), None),
        P(("row", "col"), None),
    )
    out_specs = (P(("row", "col"), "depth", None, None), P(("row", "col"), "depth", None, None))
    return jax.shard_map(local, mesh=mesh, in_specs=in_specs, out_specs=out_specs, check_vma=False)
```
